128 devices in a mesh: rows: 32 (over y_hi, z, x), tm: 4 (over y_lo, core).
Axes of the slice: x: 4, y: 4 (y_hi: 2, y_lo: 2; y = y_hi * 2 + y_lo), z: 4, core: 2. Of those that a mesh axis runs over, the one named last changes fastest.
Arguments:
- snapshots: bfloat16 [1048576, 512], P('rows', 'tm'), may hold values from -6 to 6
- modes: bfloat16 [1048576, 256], P('rows'), may hold values from -0.005859375 to 0.005859375
- eig_vectors: float32 [3, 256], replicated, may hold values from -0.375 to 0.375
- eig_values: float32 [3], replicated, may hold values from -1 to 1
Outputs:
- operator: float32 [256, 256], replicated
- eig_residual: float32 [3, 256], replicated
- residual_norm: float32 [3], replicated
The draws below stay inside these ranges and needn't reach their ends.
All inputs are finite; a program needn't handle non-finite values.
Results may differ from the reference program's by a relative error of at most 0.0003.
Values may be sent and summed in bfloat16 or wider, within the bound.
No kernel may reach another device: no remote copies, remote signals or barrier semaphores. Data moves between devices by JAX's collectives and lax.ppermute only.
A program may use at most 128 MiB of HBM per device.

```python
import jax
import jax.numpy as jnp
from jax import lax

M_DEV = 32768
R = 256
EIGS = 3
ROWS_ALL = 1048576
TIMES = 512
N_ROWS = 32


def steps_of(key, dims, shards, least, top_value):
    level = 1.0
    for position, blocks in shards:
        heights = jax.random.uniform(jax.random.fold_in(jax.random.fold_in(key, 6), position), (blocks,), jnp.float32, least / len(shards), top_value / len(shards))
        level = level * jnp.repeat(jnp.exp(heights), dims[position] // blocks).reshape((-1,) + (1,) * (len(dims) - 1 - position))
    return level


def normal_values(stream_key, dims, scale, reach, shards=(), held_as=jnp.bfloat16):
    array = scale * jax.random.normal(stream_key, dims, jnp.float32)
    if shards:
        array = array * steps_of(stream_key, dims, shards, -0.22, 0.18)
    return jnp.clip(array, -reach, reach).astype(held_as)


def setup_inputs(seed: int = 0) -> dict:
    key_of = jax.random.split(jax.random.key(seed), 5)
    snapshots = normal_values(key_of[0], (ROWS_ALL, TIMES), 1.0, 6.0, ((0, 32), (1, 4)))
    modes = normal_values(key_of[1], (ROWS_ALL, R), ROWS_ALL ** -0.5, 0.005859375, ((0, 32),))
    eig_vectors = normal_values(key_of[2], (EIGS, R), R ** -0.5, 0.375, (), jnp.float32)
    eig_values = jnp.clip(jax.random.uniform(key_of[3], (EIGS,), jnp.float32, -1.0, 1.0), -1.0, 1.0)
    return {"snapshots": snapshots, "modes": modes, "eig_vectors": eig_vectors, "eig_values": eig_values}


def reference(snapshots, modes, eig_vectors, eig_values):
    blocks_x = snapshots.reshape(N_ROWS, M_DEV, TIMES)
    blocks_u = modes.reshape(N_ROWS, M_DEV, R)

    def accumulate(total, pair):
        basis, data = pair
        term = jnp.dot(basis.astype(jnp.float32).T.astype(jnp.float32), data.astype(jnp.float32), precision=lax.Precision.HIGHEST, preferred_element_type=jnp.float32)
        return (total + term, None)
    coords, _ = lax.scan(accumulate, jnp.zeros((R, TIMES), jnp.float32), (blocks_u, blocks_x))
    lead = coords[:, :-1]
    trail = coords[:, 1:]
    scale = jnp.float32(TIMES - 1)
    cross = jnp.dot(trail.astype(jnp.float32), lead.T.astype(jnp.float32), precision=lax.Precision.HIGHEST, preferred_element_type=jnp.float32) / scale
    gram = jnp.dot(lead.astype(jnp.float32), lead.T.astype(jnp.float32), precision=lax.Precision.HIGHEST, preferred_element_type=jnp.float32) / scale + jnp.eye(R, dtype=jnp.float32)
    operator = jnp.linalg.solve(gram, cross.T).T
    eig_residual = jnp.dot(eig_vectors.astype(jnp.float32), operator.T.astype(jnp.float32), precision=lax.Precision.HIGHEST, preferred_element_type=jnp.float32) - eig_values[:, None] * eig_vectors
    residual_norm = jnp.sqrt(lax.optimization_barrier(jnp.sum(eig_residual * eig_residual, axis=1)) + 1e-06)
    return (operator, eig_residual, residual_norm)
```

```python
import functools

import jax
import jax.numpy as jnp
from jax import lax
from jax.experimental import pallas as pl
from jax.experimental.pallas import tpu as pltpu
from jax.sharding import PartitionSpec as P

LARGEST_FAST = 2048.0
RESIDUAL_FLOOR = 224.0


def pieces(array):
    high = array.astype(jnp.bfloat16)
    low = (array - high.astype(jnp.float32)).astype(jnp.bfloat16)
    return high, low


def dot3(left, right):
    left_high, left_low = left
    right_high, right_low = right
    mm = functools.partial(jnp.dot, preferred_element_type=jnp.float32)
    return mm(left_high, right_high) + (mm(left_high, right_low) + mm(left_low, right_high))


def dot_full(left, right, contract=((1,), (0,))):
    return lax.dot_general(
        left,
        right,
        (contract, ((), ())),
        precision=lax.Precision.HIGHEST,
        preferred_element_type=jnp.float32,
    )


def eliminate(gram_ref, work, width):
    lanes = lax.broadcasted_iota(jnp.int32, (1, 2 * width), 1)
    lines = lax.broadcasted_iota(jnp.int32, (width, 1), 0)

    def step(k, carry):
        row = work[pl.ds(k, 1), :]
        here = (lanes == k).astype(jnp.float32)
        pivot = jnp.sum(row * here, axis=1, keepdims=True)
        row = row / pivot
        column = jnp.sum(work[...] * here, axis=1, keepdims=True)
        on_line = lines == k
        work[...] = jnp.where(on_line, row, work[...] - column * row)
        return carry

    lax.fori_loop(0, width, step, 0)


def solve_kernel(core_ref, own_ref, other_ref, vec_ref, val_ref, op_out, res_ref, norm_ref,
                 gram_ref, cross_ref, r_ref, x_ref, op_ref, work, sem):
    width = gram_ref.shape[0]
    first = core_ref[0] == 0
    blocks = []
    for half in range(2):
        own = own_ref[:, half].reshape(width, 128)
        other = other_ref[:, half].reshape(width, 128)
        blocks.append(jnp.where(first, own, other))
        blocks.append(jnp.where(first, other, own))
    series = jnp.concatenate(blocks, axis=1)
    total = series.shape[1]
    scale = 1.0 / (total - 1)
    column = lax.broadcasted_iota(jnp.int32, (1, total), 1)
    lead = jnp.where(column < total - 1, series, 0.0)
    trail = pltpu.roll(series, total - 1, 1)
    both = dot_full(jnp.concatenate([lead, trail], axis=0), lead, ((1,), (1,)))
    eye = (
        lax.broadcasted_iota(jnp.int32, (width, width), 0)
        == lax.broadcasted_iota(jnp.int32, (width, width), 1)
    ).astype(jnp.float32)
    gram = both[:width] * scale + eye
    cross = both[width:] * scale
    gram_ref[...] = gram
    cross_ref[...] = cross

    gram_pieces = pieces(gram)
    square = dot3(gram_pieces, gram_pieces)
    top = jnp.max(jnp.sum(jnp.abs(square), axis=0, keepdims=True))
    top = jnp.maximum(jnp.sqrt(jnp.full((8, 128), top, jnp.float32)) * 1.001, 1.5)
    bound = jnp.max(top)

    @pl.when(bound <= LARGEST_FAST)
    def _():
        alpha = 2.0 / (top + 1.0)
        t1 = (top + 1.0) / (top - 1.0)
        t2 = 2.0 * t1 * t1 - 1.0
        inv2 = 1.0 / t2
        a = alpha[:1, :1]
        i2 = inv2[:1, :1]
        c = 1.0 + i2
        r_ref[...] = c * (eye - (2.0 * a) * gram_ref[...] + (a * a) * square) - i2 * eye
        x_ref[...] = (c * a) * (2.0 * eye - a * gram_ref[...])

        def more(state):
            return jnp.max(2.0 * state * state - 1.0) < RESIDUAL_FLOOR

        def double(t):
            t = 2.0 * t * t - 1.0
            it = (1.0 / t)[:1, :1]
            r = r_ref[...]
            x = x_ref[...]
            rp = pieces(r)
            x_ref[...] = (1.0 + it) * (x + dot3(pieces(x), rp))
            r_ref[...] = (1.0 + it) * dot3(rp, rp) - it * eye
            return t

        t = lax.while_loop(more, double, t2)
        t = 2.0 * t * t - 1.0
        it = (1.0 / t)[:1, :1]
        x = x_ref[...]
        x = (1.0 + it) * (x + dot3(pieces(x), pieces(r_ref[...])))
        xp = pieces(x)
        x_ref[...] = x

        def refine(guess):
            rest = cross_ref[...] - dot_full(guess, gram_ref[...])
            return guess + dot3(pieces(rest), xp)

        last = 1.0 + (1.0 / (2.0 * t * t - 1.0))[:1, :1]
        guess = dot3(pieces(cross_ref[...]), xp)
        op_ref[...] = last * refine(guess)

        @pl.when(bound > 32.0)
        def _():
            for _ in range(3):
                op_ref[...] = refine(op_ref[...])

    @pl.when(bound > LARGEST_FAST)
    def _():
        work[:, :width] = gram_ref[...]
        work[:, width:] = cross_ref[...].T
        eliminate(gram_ref, work, width)
        op_ref[...] = work[:, width:].T

    out = pltpu.make_async_copy(op_ref, op_out, sem)
    out.start()
    vectors = vec_ref[...]
    residual = dot_full(vectors, op_ref[...], ((1,), (1,))) - val_ref[...] * vectors
    res_ref[...] = residual
    norm_ref[...] = jnp.sqrt(jnp.sum(residual * residual, axis=1, keepdims=True) + 1e-06)
    out.wait()


def solve(core, own, other, vectors, values):
    eigs, width = vectors.shape
    vmem = pl.BlockSpec(memory_space=pltpu.VMEM)
    square = pltpu.VMEM((width, width), jnp.float32)
    operator, residual, norm = pl.pallas_call(
        solve_kernel,
        out_shape=(
            jax.ShapeDtypeStruct((width, width), jnp.float32),
            jax.ShapeDtypeStruct((eigs, width), jnp.float32),
            jax.ShapeDtypeStruct((eigs, 1), jnp.float32),
        ),
        in_specs=[pl.BlockSpec(memory_space=pltpu.SMEM), vmem, vmem, vmem, vmem],
        out_specs=(pl.BlockSpec(memory_space=pl.ANY), vmem, vmem),
        scratch_shapes=[square] * 5
        + [pltpu.VMEM((width, 2 * width), jnp.float32), pltpu.SemaphoreType.DMA],
        name="solve",
    )(core, own, other, vectors, values[:, None])
    return operator, residual, norm[:, 0]


def joint_groups():
    rows, halves = 32, 2
    return [[r * 4 + 2 * half + core for r in range(rows) for half in range(halves)] for core in range(2)]


def body(snapshots, modes, eig_vectors, eig_values):
    width = modes.shape[1]
    block_cols = snapshots.shape[1]
    rows = lax.axis_size("rows")
    partial_value = jnp.einsum("mr,mt->rt", modes, snapshots, preferred_element_type=jnp.float32)
    lines = width // rows
    arrived = lax.all_to_all(
        partial_value.reshape(rows, lines, block_cols), "rows", 0, 0, tiled=True
    )
    own_lines = jnp.sum(arrived, axis=0)
    axes = ("rows", "tm")
    gathered = lax.all_to_all(
        jnp.broadcast_to(own_lines[None], (2 * rows, lines, block_cols)),
        axes,
        0,
        0,
        tiled=True,
        axis_index_groups=joint_groups(),
    )
    swap = [(i, i ^ 1) for i in range(4 * rows)]
    other = lax.ppermute(gathered, axes, swap)
    core = (lax.axis_index("tm") % 2).astype(jnp.int32).reshape(1)
    shape = (rows, 2, lines, block_cols)
    return solve(core, gathered.reshape(shape), other.reshape(shape), eig_vectors, eig_values)


def solution(mesh):
    return jax.shard_map(
        body,
        mesh=mesh,
        in_specs=(P("rows", "tm"), P("rows", None), P(), P()),
        out_specs=(P(), P(), P()),
        check_vma=False,
    )
```

```python
import functools

import jax
import jax.numpy as jnp
from jax import lax
from jax.experimental import pallas as pl
from jax.experimental.pallas import tpu as pltpu
from jax.sharding import PartitionSpec as P

LARGEST_FAST = 2048.0
RESIDUAL_FLOOR = 224.0


def pieces(array):
    high = array.astype(jnp.bfloat16)
    low = (array - high.astype(jnp.float32)).astype(jnp.bfloat16)
    return high, low


def dot3(left, right):
    left_high, left_low = left
    right_high, right_low = right
    mm = functools.partial(jnp.dot, preferred_element_type=jnp.float32)
    return mm(left_high, right_high) + (mm(left_high, right_low) + mm(left_low, right_high))


def dot_full(left, right, contract=((1,), (0,))):
    return lax.dot_general(
        left,
        right,
        (contract, ((), ())),
        precision=lax.Precision.HIGHEST,
        preferred_element_type=jnp.float32,
    )


def eliminate(gram_ref, work, width):
    lanes = lax.broadcasted_iota(jnp.int32, (1, 2 * width), 1)
    lines = lax.broadcasted_iota(jnp.int32, (width, 1), 0)

    def step(k, carry):
        row = work[pl.ds(k, 1), :]
        here = (lanes == k).astype(jnp.float32)
        pivot = jnp.sum(row * here, axis=1, keepdims=True)
        row = row / pivot
        column = jnp.sum(work[...] * here, axis=1, keepdims=True)
        on_line = lines == k
        work[...] = jnp.where(on_line, row, work[...] - column * row)
        return carry

    lax.fori_loop(0, width, step, 0)


def solve_kernel(core_of, own_ref, other_ref, vec_ref, val_ref, op_out, res_ref, norm_ref,
                 gram_ref, cross_ref, r_ref, x_ref, op_ref, work, sem):
    width = gram_ref.shape[0]
    first = core_of() == 0
    blocks = []
    for half in range(2):
        own = own_ref[:, half].reshape(width, 128)
        other = other_ref[:, half].reshape(width, 128)
        blocks.append(jnp.where(first, own, other))
        blocks.append(jnp.where(first, other, own))
    series = jnp.concatenate(blocks, axis=1)
    total = series.shape[1]
    scale = 1.0 / (total - 1)
    column = lax.broadcasted_iota(jnp.int32, (1, total), 1)
    lead = jnp.where(column < total - 1, series, 0.0)
    trail = pltpu.roll(series, total - 1, 1)
    both = dot_full(jnp.concatenate([lead, trail], axis=0), lead, ((1,), (1,)))
    eye = (
        lax.broadcasted_iota(jnp.int32, (width, width), 0)
        == lax.broadcasted_iota(jnp.int32, (width, width), 1)
    ).astype(jnp.float32)
    gram = both[:width] * scale + eye
    cross = both[width:] * scale
    gram_ref[...] = gram
    cross_ref[...] = cross

    gram_pieces = pieces(gram)
    square = dot3(gram_pieces, gram_pieces)
    top = jnp.max(jnp.sum(jnp.abs(square), axis=0, keepdims=True))
    top = jnp.maximum(jnp.sqrt(jnp.full((8, 128), top, jnp.float32)) * 1.001, 1.5)
    bound = jnp.max(top)

    @pl.when(bound <= LARGEST_FAST)
    def _():
        alpha = 2.0 / (top + 1.0)
        t1 = (top + 1.0) / (top - 1.0)
        t2 = 2.0 * t1 * t1 - 1.0
        inv2 = 1.0 / t2
        a = alpha[:1, :1]
        i2 = inv2[:1, :1]
        c = 1.0 + i2
        r_ref[...] = c * (eye - (2.0 * a) * gram_ref[...] + (a * a) * square) - i2 * eye
        x_ref[...] = (c * a) * (2.0 * eye - a * gram_ref[...])

        def more(state):
            return jnp.max(2.0 * state * state - 1.0) < RESIDUAL_FLOOR

        def double(t):
            t = 2.0 * t * t - 1.0
            it = (1.0 / t)[:1, :1]
            r = r_ref[...]
            x = x_ref[...]
            rp = pieces(r)
            x_ref[...] = (1.0 + it) * (x + dot3(pieces(x), rp))
            r_ref[...] = (1.0 + it) * dot3(rp, rp) - it * eye
            return t

        t = lax.while_loop(more, double, t2)
        t = 2.0 * t * t - 1.0
        it = (1.0 / t)[:1, :1]
        x = x_ref[...]
        x = (1.0 + it) * (x + dot3(pieces(x), pieces(r_ref[...])))
        xp = pieces(x)
        x_ref[...] = x

        def refine(guess):
            rest = cross_ref[...] - dot_full(guess, gram_ref[...])
            return guess + dot3(pieces(rest), xp)

        last = 1.0 + (1.0 / (2.0 * t * t - 1.0))[:1, :1]
        guess = dot3(pieces(cross_ref[...]), xp)
        op_ref[...] = last * refine(guess)

        @pl.when(bound > 32.0)
        def _():
            for _ in range(3):
                op_ref[...] = refine(op_ref[...])

    @pl.when(bound > LARGEST_FAST)
    def _():
        work[:, :width] = gram_ref[...]
        work[:, width:] = cross_ref[...].T
        eliminate(gram_ref, work, width)
        op_ref[...] = work[:, width:].T

    out = pltpu.make_async_copy(op_ref, op_out, sem)
    out.start()
    vectors = vec_ref[...]
    eigs = vectors.shape[0]
    line = lax.broadcasted_iota(jnp.int32, (eigs, 1), 0)
    values = jnp.zeros((eigs, 1), jnp.float32)
    for k in range(eigs):
        values = jnp.where(line == k, val_ref[k], values)
    residual = dot_full(vectors, op_ref[...], ((1,), (1,))) - values * vectors
    res_ref[...] = residual
    squares = dot_full(jnp.ones((8, width), jnp.float32), residual * residual, ((1,), (1,)))
    norm_ref[...] = jnp.sqrt(squares[0] + 1e-06)
    out.wait()


def core_index():
    return lax.axis_index("tm") & 1


def solve(own, other, vectors, values, core_of=core_index):
    eigs, width = vectors.shape
    vmem = pl.BlockSpec(memory_space=pltpu.VMEM)
    square = pltpu.VMEM((width, width), jnp.float32)
    near = functools.partial(pltpu.with_memory_space_constraint, memory_space=pltpu.VMEM)
    return pl.pallas_call(
        functools.partial(solve_kernel, core_of),
        out_shape=(
            jax.ShapeDtypeStruct((width, width), jnp.float32),
            jax.ShapeDtypeStruct((eigs, width), jnp.float32),
            jax.ShapeDtypeStruct((eigs,), jnp.float32),
        ),
        in_specs=[vmem, vmem, vmem, pl.BlockSpec(memory_space=pltpu.SMEM)],
        out_specs=(pl.BlockSpec(memory_space=pl.ANY), vmem, vmem),
        scratch_shapes=[square] * 5
        + [pltpu.VMEM((width, 2 * width), jnp.float32), pltpu.SemaphoreType.DMA],
        compiler_params=pltpu.CompilerParams(vmem_limit_bytes=16 * 2**20),
        name="solve",
    )(near(own), near(other), vectors, values)


def project_kernel(chunk, modes_hbm, snaps_hbm, out, modes_vmem, snaps_vmem, total, mode_sem, snap_sem):
    steps = modes_hbm.shape[0] // chunk

    def copies(step):
        lines = pl.ds(step * chunk, chunk)
        return (
            pltpu.make_async_copy(modes_hbm.at[lines], modes_vmem.at[lines], mode_sem.at[step]),
            pltpu.make_async_copy(snaps_hbm.at[lines], snaps_vmem.at[lines], snap_sem.at[step]),
        )

    for step in range(steps):
        for copy in copies(step):
            copy.start()
    total[...] = jnp.zeros_like(total)

    def add(step, carry):
        for copy in copies(step):
            copy.wait()
        lines = pl.ds(pl.multiple_of(step * chunk, chunk), chunk)
        total[...] += lax.dot_general(
            snaps_vmem[lines, :],
            modes_vmem[lines, :],
            (((0,), (0,)), ((), ())),
            preferred_element_type=jnp.float32,
        )
        return carry

    lax.fori_loop(0, steps, add, 0)
    out[...] = total[...].T


def project(modes, snapshots, chunk=2048):
    width, cols = modes.shape[1], snapshots.shape[1]
    steps = modes.shape[0] // chunk
    far = functools.partial(pltpu.with_memory_space_constraint, memory_space=pltpu.HBM)
    return pl.pallas_call(
        functools.partial(project_kernel, chunk),
        out_shape=jax.ShapeDtypeStruct((width, cols), jnp.float32),
        in_specs=[pl.BlockSpec(memory_space=pltpu.HBM)] * 2,
        out_specs=pl.BlockSpec(memory_space=pltpu.VMEM),
        scratch_shapes=[
            pltpu.VMEM(modes.shape, modes.dtype),
            pltpu.VMEM(snapshots.shape, snapshots.dtype),
            pltpu.VMEM((cols, width), jnp.float32),
            pltpu.SemaphoreType.DMA((steps,)),
            pltpu.SemaphoreType.DMA((steps,)),
        ],
        compiler_params=pltpu.CompilerParams(vmem_limit_bytes=40 * 2**20),
        name="project",
    )(far(modes), far(snapshots))


def joint_groups():
    rows, halves = 32, 2
    return [[r * 4 + 2 * half + core for r in range(rows) for half in range(halves)] for core in range(2)]


def body(snapshots, modes, eig_vectors, eig_values):
    width = modes.shape[1]
    block_cols = snapshots.shape[1]
    rows = lax.axis_size("rows")
    partial_value = project(modes, snapshots)
    lines = width // rows
    arrived = lax.all_to_all(
        partial_value.reshape(rows, lines, block_cols), "rows", 0, 0, tiled=True
    )
    own_lines = jnp.sum(arrived, axis=0)
    axes = ("rows", "tm")
    gathered = lax.all_to_all(
        jnp.broadcast_to(own_lines[None], (2 * rows, lines, block_cols)),
        axes,
        0,
        0,
        tiled=True,
        axis_index_groups=joint_groups(),
    )
    swap = [(i, i ^ 1) for i in range(4 * rows)]
    other = lax.ppermute(gathered, axes, swap)
    shape = (rows, 2, lines, block_cols)
    return solve(gathered.reshape(shape), other.reshape(shape), eig_vectors, eig_values)


def solution(mesh):
    return jax.shard_map(
        body,
        mesh=mesh,
        in_specs=(P("rows", "tm"), P("rows", None), P(), P()),
        out_specs=(P(), P(), P()),
        check_vma=False,
    )
```

```python
import functools
import math

import jax
import jax.numpy as jnp
from jax import lax
from jax.experimental import pallas as pl
from jax.experimental.pallas import tpu as pltpu
from jax.sharding import PartitionSpec as P

LARGEST_FAST = 2048.0
RESIDUAL_FLOOR = 224.0


def pieces(array):
    high = array.astype(jnp.bfloat16)
    low = (array - high.astype(jnp.float32)).astype(jnp.bfloat16)
    return high, low


def dot3(left, right):
    left_high, left_low = left
    right_high, right_low = right
    mm = functools.partial(jnp.dot, preferred_element_type=jnp.float32)
    return mm(left_high, right_high) + (mm(left_high, right_low) + mm(left_low, right_high))


def dot_full(left, right, contract=((1,), (0,))):
    return lax.dot_general(
        left,
        right,
        (contract, ((), ())),
        precision=lax.Precision.HIGHEST,
        preferred_element_type=jnp.float32,
    )


def bound_for(doublings):
    t = RESIDUAL_FLOOR
    for _ in range(doublings + 1):
        t = math.sqrt((t + 1.0) / 2.0)
    return (t + 1.0) / (t - 1.0)


def eliminate(gram_ref, work, width):
    lanes = lax.broadcasted_iota(jnp.int32, (1, 2 * width), 1)
    lines = lax.broadcasted_iota(jnp.int32, (width, 1), 0)

    def step(k, carry):
        row = work[pl.ds(k, 1), :]
        here = (lanes == k).astype(jnp.float32)
        pivot = jnp.sum(row * here, axis=1, keepdims=True)
        row = row / pivot
        column = jnp.sum(work[...] * here, axis=1, keepdims=True)
        on_line = lines == k
        work[...] = jnp.where(on_line, row, work[...] - column * row)
        return carry

    lax.fori_loop(0, width, step, 0)


def core_index():
    return lax.axis_index("tm") & 1


def block_of(ref, half):
    return ref[:, half].reshape(-1, ref.shape[-1])


def half_sums(blocks, drop_last):
    cols = blocks[0].shape[1]
    column = lax.broadcasted_iota(jnp.int32, (1, cols), 1)
    inner = column < cols - 1
    leads = jnp.concatenate(
        [blocks[0], jnp.where(jnp.logical_or(inner, jnp.logical_not(drop_last)), blocks[1], 0.0)],
        axis=1,
    )
    starts = jnp.concatenate([jnp.where(inner, block, 0.0) for block in blocks], axis=1)
    nexts = jnp.concatenate([pltpu.roll(block, cols - 1, 1) for block in blocks], axis=1)
    gram = dot_full(leads, leads, ((1,), (1,)))
    cross = dot_full(nexts, starts, ((1,), (1,)))
    return gram, cross


def own_kernel(core_of, own_ref, gram_ref, cross_ref):
    blocks = [block_of(own_ref, 0), block_of(own_ref, 1)]
    gram, cross = half_sums(blocks, core_of() == 1)
    gram_ref[...] = gram
    cross_ref[...] = cross


def near(array):
    return pltpu.with_memory_space_constraint(array, pltpu.VMEM)


def own_sums(own, width, core_of=core_index):
    vmem = pl.BlockSpec(memory_space=pltpu.VMEM)
    square = jax.ShapeDtypeStruct((width, width), jnp.float32)
    return pl.pallas_call(
        functools.partial(own_kernel, core_of),
        out_shape=(square, square),
        in_specs=[vmem],
        out_specs=(vmem, vmem),
        compiler_params=pltpu.CompilerParams(vmem_limit_bytes=16 * 2**20),
        cost_estimate=pl.CostEstimate(
            flops=24 * width**3, bytes_accessed=12 * width * width, transcendentals=0
        ),
        name="own_sums",
    )(near(own))


def solve_kernel(core_of, own_ref, other_ref, gram_own_ref, cross_own_ref, vec_ref, val_ref,
                 op_out, res_out, norm_out,
                 gram_ref, cross_ref, r_ref, x_ref, op_ref, work, res_ref, norm_ref, sems):
    width = gram_ref.shape[0]
    core = core_of()
    first = core == 0
    own = [block_of(own_ref, half) for half in range(2)]
    other = [block_of(other_ref, half) for half in range(2)]
    cols = own[0].shape[1]
    scale = 1.0 / (4 * cols - 1)
    eye = (
        lax.broadcasted_iota(jnp.int32, (width, width), 0)
        == lax.broadcasted_iota(jnp.int32, (width, width), 1)
    ).astype(jnp.float32)
    gram_other, cross_other = half_sums(other, first)
    gram = (gram_own_ref[...] + gram_other) * scale + eye
    gram_ref[...] = gram
    gram_pieces = pieces(gram)
    square = dot3(gram_pieces, gram_pieces)

    lane = lax.broadcasted_iota(jnp.int32, (1, cols), 1)
    series = []
    for half in range(2):
        series.append(jnp.where(first, own[half], other[half]))
        series.append(jnp.where(first, other[half], own[half]))
    ends = jnp.zeros_like(series[0])
    begins = jnp.zeros_like(series[0])
    for k in range(3):
        ends = jnp.where(lane == k, pltpu.roll(series[k], k + 1, 1), ends)
        begin = series[k + 1] if k == 0 else pltpu.roll(series[k + 1], k, 1)
        begins = jnp.where(lane == k, begin, begins)
    edges = dot_full(begins, ends, ((1,), (1,)))
    cross_ref[...] = (cross_own_ref[...] + cross_other + edges) * scale

    vectors = vec_ref[...]
    eigs = vectors.shape[0]
    on_diagonal = (
        lax.broadcasted_iota(jnp.int32, (eigs, eigs), 0)
        == lax.broadcasted_iota(jnp.int32, (eigs, eigs), 1)
    )
    values = jnp.sum(jnp.where(on_diagonal, val_ref[...][None, :], 0.0), axis=1, keepdims=True)

    top = jnp.max(jnp.sum(jnp.abs(square), axis=0, keepdims=True), axis=1, keepdims=True)
    bound_squared = top[0, 0]
    top = jnp.maximum(jnp.sqrt(top) * 1.001, 1.5)
    doublings = jnp.int32(0)
    for k in range(1, 8):
        doublings += (bound_squared > (bound_for(k) / 1.001) ** 2).astype(jnp.int32)

    @pl.when(bound_squared <= LARGEST_FAST**2)
    def _():
        alpha = 2.0 / (top + 1.0)
        t1 = (top + 1.0) / (top - 1.0)
        t2 = 2.0 * t1 * t1 - 1.0
        i2 = 1.0 / t2
        c = 1.0 + i2
        r_ref[...] = c * (eye - (2.0 * alpha) * gram_ref[...] + (alpha * alpha) * square) - i2 * eye
        x_ref[...] = (c * alpha) * (2.0 * eye - alpha * gram_ref[...])

        def double(_, t):
            t = 2.0 * t * t - 1.0
            it = 1.0 / t
            x = x_ref[...]
            rp = pieces(r_ref[...])
            x_ref[...] = (1.0 + it) * (x + dot3(pieces(x), rp))
            r_ref[...] = (1.0 + it) * dot3(rp, rp) - it * eye
            return t

        t = lax.fori_loop(0, doublings, double, t2)
        t = 2.0 * t * t - 1.0
        x = x_ref[...]
        x = (1.0 + 1.0 / t) * (x + dot3(pieces(x), pieces(r_ref[...])))
        x_ref[...] = x
        xp = pieces(x)

        def refine(guess, xp):
            rest = cross_ref[...] - dot_full(guess, gram_ref[...])
            return guess + dot3(pieces(rest), xp)

        last = 1.0 + 1.0 / (2.0 * t * t - 1.0)
        op_ref[...] = last * refine(dot3(pieces(cross_ref[...]), xp), xp)

        def again(_, carry):
            op_ref[...] = refine(op_ref[...], pieces(x_ref[...]))
            return carry

        lax.fori_loop(0, jnp.where(bound_squared > 32.0**2, 3, 0), again, 0)

    @pl.when(bound_squared > LARGEST_FAST**2)
    def _():
        work[:, :width] = gram_ref[...]
        work[:, width:] = cross_ref[...].T
        eliminate(gram_ref, work, width)
        op_ref[...] = work[:, width:].T

    out = pltpu.make_async_copy(op_ref, op_out, sems.at[0])
    out.start()
    residual = dot_full(vectors, op_ref[...], ((1,), (1,))) - values * vectors
    res_ref[...] = residual
    res = pltpu.make_async_copy(res_ref, res_out, sems.at[1])
    res.start()
    squares = dot_full(jnp.ones((8, width), jnp.float32), residual * residual, ((1,), (1,)))
    norm_ref[...] = jnp.sqrt(squares[0] + 1e-06)
    norm = pltpu.make_async_copy(norm_ref, norm_out, sems.at[2])
    norm.start()
    out.wait()
    res.wait()
    norm.wait()


def solve(own, other, gram_own, cross_own, vectors, values, core_of=core_index):
    eigs, width = vectors.shape
    vmem = pl.BlockSpec(memory_space=pltpu.VMEM)
    hbm = pl.BlockSpec(memory_space=pltpu.HBM)
    square = pltpu.VMEM((width, width), jnp.float32)
    return pl.pallas_call(
        functools.partial(solve_kernel, core_of),
        out_shape=(
            jax.ShapeDtypeStruct((width, width), jnp.float32),
            jax.ShapeDtypeStruct((eigs, width), jnp.float32),
            jax.ShapeDtypeStruct((eigs,), jnp.float32),
        ),
        in_specs=[vmem] * 6,
        out_specs=(hbm, hbm, hbm),
        scratch_shapes=[square] * 5
        + [
            pltpu.VMEM((width, 2 * width), jnp.float32),
            pltpu.VMEM((eigs, width), jnp.float32),
            pltpu.VMEM((eigs,), jnp.float32),
            pltpu.SemaphoreType.DMA((3,)),
        ],
        compiler_params=pltpu.CompilerParams(vmem_limit_bytes=16 * 2**20),
        name="solve",
    )(*map(near, (own, other, gram_own, cross_own, vectors, values)))


def project_kernel(chunk, modes_hbm, snaps_hbm, out, modes_vmem, snaps_vmem, total, mode_sem, snap_sem):
    steps = modes_hbm.shape[0] // chunk

    def copies(step):
        lines = pl.ds(step * chunk, chunk)
        return (
            pltpu.make_async_copy(modes_hbm.at[lines], modes_vmem.at[lines], mode_sem.at[step]),
            pltpu.make_async_copy(snaps_hbm.at[lines], snaps_vmem.at[lines], snap_sem.at[step]),
        )

    for step in range(steps):
        for copy in copies(step):
            copy.start()
    total[...] = jnp.zeros_like(total)

    def add(step, carry):
        for copy in copies(step):
            copy.wait()
        lines = pl.ds(pl.multiple_of(step * chunk, chunk), chunk)
        total[...] += lax.dot_general(
            snaps_vmem[lines, :],
            modes_vmem[lines, :],
            (((0,), (0,)), ((), ())),
            preferred_element_type=jnp.float32,
        )
        return carry

    lax.fori_loop(0, steps, add, 0)
    out[...] = total[...].T


def project(modes, snapshots, chunk=2048):
    width, cols = modes.shape[1], snapshots.shape[1]
    steps = modes.shape[0] // chunk
    far = functools.partial(pltpu.with_memory_space_constraint, memory_space=pltpu.HBM)
    return pl.pallas_call(
        functools.partial(project_kernel, chunk),
        out_shape=jax.ShapeDtypeStruct((width, cols), jnp.float32),
        in_specs=[pl.BlockSpec(memory_space=pltpu.HBM)] * 2,
        out_specs=pl.BlockSpec(memory_space=pltpu.VMEM),
        scratch_shapes=[
            pltpu.VMEM(modes.shape, modes.dtype),
            pltpu.VMEM(snapshots.shape, snapshots.dtype),
            pltpu.VMEM((cols, width), jnp.float32),
            pltpu.SemaphoreType.DMA((steps,)),
            pltpu.SemaphoreType.DMA((steps,)),
        ],
        compiler_params=pltpu.CompilerParams(vmem_limit_bytes=40 * 2**20),
        name="project",
    )(far(modes), far(snapshots))


def joint_groups():
    rows, halves = 32, 2
    return [[r * 4 + 2 * half + core for r in range(rows) for half in range(halves)] for core in range(2)]


def body(snapshots, modes, eig_vectors, eig_values):
    width = modes.shape[1]
    block_cols = snapshots.shape[1]
    rows = lax.axis_size("rows")
    partial_value = project(modes, snapshots)
    lines = width // rows
    arrived = lax.all_to_all(
        partial_value.reshape(rows, lines, block_cols), "rows", 0, 0, tiled=True
    )
    own_lines = jnp.sum(arrived, axis=0)
    axes = ("rows", "tm")
    gathered = lax.all_to_all(
        jnp.broadcast_to(own_lines[None], (2 * rows, lines, block_cols)),
        axes,
        0,
        0,
        tiled=True,
        axis_index_groups=joint_groups(),
    )
    swap = [(i, i ^ 1) for i in range(4 * rows)]
    other = lax.ppermute(gathered, axes, swap)
    shape = (rows, 2, lines, block_cols)
    own, other = gathered.reshape(shape), other.reshape(shape)
    gram_own, cross_own = own_sums(own, width)
    return solve(own, other, gram_own, cross_own, eig_vectors, eig_values)


def solution(mesh):
    return jax.shard_map(
        body,
        mesh=mesh,
        in_specs=(P("rows", "tm"), P("rows", None), P(), P()),
        out_specs=(P(), P(), P()),
        check_vma=False,
    )
```

```python
import functools
import math

import jax
import jax.numpy as jnp
from jax import lax
from jax.experimental import pallas as pl
from jax.experimental.pallas import tpu as pltpu
from jax.sharding import PartitionSpec as P

LARGEST_FAST = 2048.0
RESIDUAL_FLOOR = 224.0
PLAIN = ((1,), (0,))
ACROSS = ((1,), (1,))


def pieces(array):
    high = array.astype(jnp.bfloat16)
    low = (array - high.astype(jnp.float32)).astype(jnp.bfloat16)
    return high, low


def dot3(left, right, contract=PLAIN):
    left_high, left_low = left
    right_high, right_low = right

    def mm(a, b):
        return lax.dot_general(a, b, (contract, ((), ())), preferred_element_type=jnp.float32)

    return mm(left_high, right_high) + (mm(left_high, right_low) + mm(left_low, right_high))


def dot_full(left, right, contract=PLAIN):
    return lax.dot_general(
        left,
        right,
        (contract, ((), ())),
        precision=lax.Precision.HIGHEST,
        preferred_element_type=jnp.float32,
    )


def bound_for(doublings):
    t = RESIDUAL_FLOOR
    for _ in range(doublings + 1):
        t = math.sqrt((t + 1.0) / 2.0)
    return (t + 1.0) / (t - 1.0)


def eliminate(gram_ref, work, width):
    lanes = lax.broadcasted_iota(jnp.int32, (1, 2 * width), 1)
    lines = lax.broadcasted_iota(jnp.int32, (width, 1), 0)

    def step(k, carry):
        row = work[pl.ds(k, 1), :]
        here = (lanes == k).astype(jnp.float32)
        pivot = jnp.sum(row * here, axis=1, keepdims=True)
        row = row / pivot
        column = jnp.sum(work[...] * here, axis=1, keepdims=True)
        on_line = lines == k
        work[...] = jnp.where(on_line, row, work[...] - column * row)
        return carry

    lax.fori_loop(0, width, step, 0)


def core_index():
    return lax.axis_index("tm") & 1


def block_of(ref, half):
    return ref[:, half].reshape(-1, ref.shape[-1])


def half_sums(blocks, drop_last):
    cols = blocks[0].shape[1]
    column = lax.broadcasted_iota(jnp.int32, (1, cols), 1)
    inner = column < cols - 1
    leads = jnp.concatenate(
        [blocks[0], jnp.where(jnp.logical_or(inner, jnp.logical_not(drop_last)), blocks[1], 0.0)],
        axis=1,
    )
    starts = jnp.concatenate([jnp.where(inner, block, 0.0) for block in blocks], axis=1)
    nexts = jnp.concatenate([pltpu.roll(block, cols - 1, 1) for block in blocks], axis=1)
    gram = dot_full(leads, leads, ACROSS)
    cross = dot_full(nexts, starts, ACROSS)
    return gram, cross


def own_kernel(core_of, own_ref, gram_ref, cross_ref):
    blocks = [block_of(own_ref, 0), block_of(own_ref, 1)]
    gram, cross = half_sums(blocks, core_of() == 1)
    gram_ref[...] = gram
    cross_ref[...] = cross


def near(array):
    return pltpu.with_memory_space_constraint(array, pltpu.VMEM)


def own_sums(own, width, core_of=core_index):
    vmem = pl.BlockSpec(memory_space=pltpu.VMEM)
    square = jax.ShapeDtypeStruct((width, width), jnp.float32)
    return pl.pallas_call(
        functools.partial(own_kernel, core_of),
        out_shape=(square, square),
        in_specs=[vmem],
        out_specs=(vmem, vmem),
        compiler_params=pltpu.CompilerParams(vmem_limit_bytes=16 * 2**20),
        cost_estimate=pl.CostEstimate(
            flops=24 * width**3, bytes_accessed=12 * width * width, transcendentals=0
        ),
        name="own_sums",
    )(near(own))


def solve_kernel(core_of, own_ref, other_ref, gram_own_ref, cross_own_ref, vec_ref, val_ref,
                 op_out, res_out, norm_out,
                 gram_ref, cross_ref, r_ref, x_ref, op_ref, work, seen_ref, res_ref, norm_ref, sems):
    width = gram_ref.shape[0]
    core = core_of()
    first = core == 0
    own = [block_of(own_ref, half) for half in range(2)]
    other = [block_of(other_ref, half) for half in range(2)]
    cols = own[0].shape[1]
    scale = 1.0 / (4 * cols - 1)
    eye = (
        lax.broadcasted_iota(jnp.int32, (width, width), 0)
        == lax.broadcasted_iota(jnp.int32, (width, width), 1)
    ).astype(jnp.float32)
    gram_other, cross_other = half_sums(other, first)
    gram = (gram_own_ref[...] + gram_other) * scale + eye
    gram_ref[...] = gram
    gram_pieces = pieces(gram)
    square = dot3(gram_pieces, gram_pieces)

    lane = lax.broadcasted_iota(jnp.int32, (1, cols), 1)
    series = []
    for half in range(2):
        series.append(jnp.where(first, own[half], other[half]))
        series.append(jnp.where(first, other[half], own[half]))
    ends = jnp.zeros_like(series[0])
    begins = jnp.zeros_like(series[0])
    for k in range(3):
        ends = jnp.where(lane == k, pltpu.roll(series[k], k + 1, 1), ends)
        begin = series[k + 1] if k == 0 else pltpu.roll(series[k + 1], k, 1)
        begins = jnp.where(lane == k, begin, begins)
    edges = dot_full(begins, ends, ACROSS)
    cross_ref[...] = (cross_own_ref[...] + cross_other + edges) * scale

    vectors = vec_ref[...]
    eigs = vectors.shape[0]
    on_diagonal = (
        lax.broadcasted_iota(jnp.int32, (eigs, eigs), 0)
        == lax.broadcasted_iota(jnp.int32, (eigs, eigs), 1)
    )
    values = jnp.sum(jnp.where(on_diagonal, val_ref[...][None, :], 0.0), axis=1, keepdims=True)

    top = jnp.max(jnp.sum(jnp.abs(square), axis=0, keepdims=True), axis=1, keepdims=True)
    bound_squared = top[0, 0]
    top = jnp.maximum(jnp.sqrt(top) * 1.001, 1.5)
    doublings = jnp.int32(0)
    for k in range(1, 8):
        doublings += (bound_squared > (bound_for(k) / 1.001) ** 2).astype(jnp.int32)

    @pl.when(bound_squared <= LARGEST_FAST**2)
    def _():
        alpha = 2.0 / (top + 1.0)
        t1 = (top + 1.0) / (top - 1.0)
        t2 = 2.0 * t1 * t1 - 1.0
        i2 = 1.0 / t2
        c = 1.0 + i2
        r_ref[...] = c * (eye - (2.0 * alpha) * gram_ref[...] + (alpha * alpha) * square) - i2 * eye
        x_ref[...] = (c * alpha) * (2.0 * eye - alpha * gram_ref[...])

        def double(_, t):
            t = 2.0 * t * t - 1.0
            it = 1.0 / t
            x = x_ref[...]
            rp = pieces(r_ref[...])
            x_ref[...] = (1.0 + it) * (x + dot3(pieces(x), rp))
            r_ref[...] = (1.0 + it) * dot3(rp, rp) - it * eye
            return t

        t = lax.fori_loop(0, doublings, double, t2)
        t = 2.0 * t * t - 1.0
        x = x_ref[...]
        x = (1.0 + 1.0 / t) * (x + dot3(pieces(x), pieces(r_ref[...])))
        x_ref[...] = x
        xp = pieces(x)

        guess = dot3(pieces(cross_ref[...]), xp)
        seen = dot_full(vectors, guess, ACROSS)
        mixed = dot3(pieces(vectors), xp, ACROSS)
        rest = pieces(cross_ref[...] - dot_full(guess, gram_ref[...]))
        last = 1.0 + 1.0 / (2.0 * t * t - 1.0)
        op_ref[...] = last * (guess + dot3(rest, xp))
        seen_ref[...] = last * (seen + dot3(pieces(mixed), rest, ACROSS))

    @pl.when(jnp.logical_and(bound_squared > 32.0**2, bound_squared <= LARGEST_FAST**2))
    def _():
        def again(_, carry):
            guess = op_ref[...]
            rest = cross_ref[...] - dot_full(guess, gram_ref[...])
            op_ref[...] = guess + dot3(pieces(rest), pieces(x_ref[...]))
            return carry

        lax.fori_loop(0, 3, again, 0)

    @pl.when(bound_squared > LARGEST_FAST**2)
    def _():
        work[:, :width] = gram_ref[...]
        work[:, width:] = cross_ref[...].T
        eliminate(gram_ref, work, width)
        op_ref[...] = work[:, width:].T

    out = pltpu.make_async_copy(op_ref, op_out, sems.at[0])
    out.start()

    @pl.when(bound_squared > 32.0**2)
    def _():
        seen_ref[...] = dot_full(vectors, op_ref[...], ACROSS)

    residual = seen_ref[...] - values * vectors
    res_ref[...] = residual
    res = pltpu.make_async_copy(res_ref, res_out, sems.at[1])
    res.start()
    sums = jnp.sum(residual * residual, axis=1, keepdims=True)
    sums = jnp.sum(jnp.where(on_diagonal, sums, 0.0), axis=0)
    norm_ref[...] = jnp.sqrt(sums + 1e-06)
    norm = pltpu.make_async_copy(norm_ref, norm_out, sems.at[2])
    norm.start()
    out.wait()
    res.wait()
    norm.wait()


def solve(own, other, gram_own, cross_own, vectors, values, core_of=core_index):
    eigs, width = vectors.shape
    vmem = pl.BlockSpec(memory_space=pltpu.VMEM)
    hbm = pl.BlockSpec(memory_space=pltpu.HBM)
    square = pltpu.VMEM((width, width), jnp.float32)
    return pl.pallas_call(
        functools.partial(solve_kernel, core_of),
        out_shape=(
            jax.ShapeDtypeStruct((width, width), jnp.float32),
            jax.ShapeDtypeStruct((eigs, width), jnp.float32),
            jax.ShapeDtypeStruct((eigs,), jnp.float32),
        ),
        in_specs=[vmem] * 6,
        out_specs=(hbm, hbm, hbm),
        scratch_shapes=[square] * 5
        + [
            pltpu.VMEM((width, 2 * width), jnp.float32),
            pltpu.VMEM((eigs, width), jnp.float32),
            pltpu.VMEM((eigs, width), jnp.float32),
            pltpu.VMEM((eigs,), jnp.float32),
            pltpu.SemaphoreType.DMA((3,)),
        ],
        compiler_params=pltpu.CompilerParams(vmem_limit_bytes=16 * 2**20),
        name="solve",
    )(*map(near, (own, other, gram_own, cross_own, vectors, values)))


def project_kernel(chunk, modes_hbm, snaps_hbm, out, modes_vmem, snaps_vmem, total, mode_sem, snap_sem):
    steps = modes_hbm.shape[0] // chunk
    tail = chunk // 2

    def copies(step, start, size):
        lines = pl.ds(start, size)
        return (
            pltpu.make_async_copy(modes_hbm.at[lines], modes_vmem.at[lines], mode_sem.at[step]),
            pltpu.make_async_copy(snaps_hbm.at[lines], snaps_vmem.at[lines], snap_sem.at[step]),
        )

    pieces_of = [(step, step * chunk, chunk) for step in range(steps - 1)]
    pieces_of += [(steps - 1 + k, (steps - 1) * chunk + k * tail, tail) for k in range(2)]
    for piece in pieces_of:
        for copy in copies(*piece):
            copy.start()

    def product(step, start, size):
        for copy in copies(step, start, size):
            copy.wait()
        lines = pl.ds(start, size)
        return lax.dot_general(
            snaps_vmem[lines, :],
            modes_vmem[lines, :],
            (((0,), (0,)), ((), ())),
            preferred_element_type=jnp.float32,
        )

    total[...] = product(0, 0, chunk)

    def add(step, carry):
        total[...] += product(step, pl.multiple_of(step * chunk, chunk), chunk)
        return carry

    lax.fori_loop(1, steps - 1, add, 0)
    total[...] += product(*pieces_of[-2])
    out[...] = (total[...] + product(*pieces_of[-1])).T


def project(modes, snapshots, chunk=2048):
    width, cols = modes.shape[1], snapshots.shape[1]
    steps = modes.shape[0] // chunk + 1
    far = functools.partial(pltpu.with_memory_space_constraint, memory_space=pltpu.HBM)
    return pl.pallas_call(
        functools.partial(project_kernel, chunk),
        out_shape=jax.ShapeDtypeStruct((width, cols), jnp.float32),
        in_specs=[pl.BlockSpec(memory_space=pltpu.HBM)] * 2,
        out_specs=pl.BlockSpec(memory_space=pltpu.VMEM),
        scratch_shapes=[
            pltpu.VMEM(modes.shape, modes.dtype),
            pltpu.VMEM(snapshots.shape, snapshots.dtype),
            pltpu.VMEM((cols, width), jnp.float32),
            pltpu.SemaphoreType.DMA((steps,)),
            pltpu.SemaphoreType.DMA((steps,)),
        ],
        compiler_params=pltpu.CompilerParams(vmem_limit_bytes=40 * 2**20),
        name="project",
    )(far(modes), far(snapshots))


def joint_groups():
    rows, halves = 32, 2
    return [[r * 4 + 2 * half + core for r in range(rows) for half in range(halves)] for core in range(2)]


def body(snapshots, modes, eig_vectors, eig_values):
    width = modes.shape[1]
    block_cols = snapshots.shape[1]
    rows = lax.axis_size("rows")
    partial_value = project(modes, snapshots)
    lines = width // rows
    arrived = lax.all_to_all(
        partial_value.reshape(rows, lines, block_cols), "rows", 0, 0, tiled=True
    )
    own_lines = jnp.sum(arrived, axis=0)
    axes = ("rows", "tm")
    gathered = lax.all_to_all(
        jnp.broadcast_to(own_lines[None], (2 * rows, lines, block_cols)),
        axes,
        0,
        0,
        tiled=True,
        axis_index_groups=joint_groups(),
    )
    swap = [(i, i ^ 1) for i in range(4 * rows)]
    other = lax.ppermute(gathered, axes, swap)
    shape = (rows, 2, lines, block_cols)
    own, other = gathered.reshape(shape), other.reshape(shape)
    gram_own, cross_own = own_sums(own, width)
    return solve(own, other, gram_own, cross_own, eig_vectors, eig_values)


def solution(mesh):
    return jax.shard_map(
        body,
        mesh=mesh,
        in_specs=(P("rows", "tm"), P("rows", None), P(), P()),
        out_specs=(P(), P(), P()),
        check_vma=False,
    )
```

```python
import functools
import math

import jax
import jax.numpy as jnp
from jax import lax
from jax.experimental import pallas as pl
from jax.experimental.pallas import tpu as pltpu
from jax.sharding import PartitionSpec as P

LARGEST_FAST = 2048.0
RESIDUAL_FLOOR = 150.0
PLAIN = ((1,), (0,))
ACROSS = ((1,), (1,))


def pieces(array):
    high = array.astype(jnp.bfloat16)
    low = (array - high.astype(jnp.float32)).astype(jnp.bfloat16)
    return high, low


def dot3(left, right, contract=PLAIN):
    left_high, left_low = left
    right_high, right_low = right

    def mm(a, b):
        return lax.dot_general(a, b, (contract, ((), ())), preferred_element_type=jnp.float32)

    return mm(left_high, right_high) + (mm(left_high, right_low) + mm(left_low, right_high))


def dot_full(left, right, contract=PLAIN):
    return lax.dot_general(
        left,
        right,
        (contract, ((), ())),
        precision=lax.Precision.HIGHEST,
        preferred_element_type=jnp.float32,
    )


def bound_for(doublings):
    t = RESIDUAL_FLOOR
    for _ in range(doublings + 1):
        t = math.sqrt((t + 1.0) / 2.0)
    return (t + 1.0) / (t - 1.0)


def eliminate(gram_ref, work, width):
    lanes = lax.broadcasted_iota(jnp.int32, (1, 2 * width), 1)
    lines = lax.broadcasted_iota(jnp.int32, (width, 1), 0)

    def step(k, carry):
        row = work[pl.ds(k, 1), :]
        here = (lanes == k).astype(jnp.float32)
        pivot = jnp.sum(row * here, axis=1, keepdims=True)
        row = row / pivot
        column = jnp.sum(work[...] * here, axis=1, keepdims=True)
        on_line = lines == k
        work[...] = jnp.where(on_line, row, work[...] - column * row)
        return carry

    lax.fori_loop(0, width, step, 0)


def core_index():
    return lax.axis_index("tm") & 1


def block_of(ref, half):
    return ref[:, half].reshape(-1, ref.shape[-1])


def half_sums(blocks, drop_last):
    cols = blocks[0].shape[1]
    column = lax.broadcasted_iota(jnp.int32, (1, cols), 1)
    inner = column < cols - 1
    leads = jnp.concatenate(
        [blocks[0], jnp.where(jnp.logical_or(inner, jnp.logical_not(drop_last)), blocks[1], 0.0)],
        axis=1,
    )
    starts = jnp.concatenate([jnp.where(inner, block, 0.0) for block in blocks], axis=1)
    nexts = jnp.concatenate([pltpu.roll(block, cols - 1, 1) for block in blocks], axis=1)
    gram = dot_full(leads, leads, ACROSS)
    cross = dot_full(nexts, starts, ACROSS)
    return gram, cross


def own_kernel(core_of, own_ref, gram_ref, cross_ref):
    blocks = [block_of(own_ref, 0), block_of(own_ref, 1)]
    gram, cross = half_sums(blocks, core_of() == 1)
    gram_ref[...] = gram
    cross_ref[...] = cross


def near(array):
    return pltpu.with_memory_space_constraint(array, pltpu.VMEM)


def own_sums(own, width, core_of=core_index):
    vmem = pl.BlockSpec(memory_space=pltpu.VMEM)
    square = jax.ShapeDtypeStruct((width, width), jnp.float32)
    return pl.pallas_call(
        functools.partial(own_kernel, core_of),
        out_shape=(square, square),
        in_specs=[vmem],
        out_specs=(vmem, vmem),
        compiler_params=pltpu.CompilerParams(vmem_limit_bytes=16 * 2**20),
        cost_estimate=pl.CostEstimate(
            flops=24 * width**3, bytes_accessed=12 * width * width, transcendentals=0
        ),
        name="own_sums",
    )(near(own))


def solve_kernel(core_of, own_ref, other_ref, gram_own_ref, cross_own_ref, vec_ref, val_ref,
                 op_out, res_out, norm_out,
                 gram_ref, cross_ref, r_ref, x_ref, op_ref, work, seen_ref, res_ref, norm_ref, sems):
    width = gram_ref.shape[0]
    core = core_of()
    first = core == 0
    own = [block_of(own_ref, half) for half in range(2)]
    other = [block_of(other_ref, half) for half in range(2)]
    cols = own[0].shape[1]
    scale = 1.0 / (4 * cols - 1)
    eye = (
        lax.broadcasted_iota(jnp.int32, (width, width), 0)
        == lax.broadcasted_iota(jnp.int32, (width, width), 1)
    ).astype(jnp.float32)
    gram_other, cross_other = half_sums(other, first)
    gram = (gram_own_ref[...] + gram_other) * scale + eye
    gram_ref[...] = gram
    gram_pieces = pieces(gram)
    square = dot3(gram_pieces, gram_pieces)

    lane = lax.broadcasted_iota(jnp.int32, (1, cols), 1)
    series = []
    for half in range(2):
        series.append(jnp.where(first, own[half], other[half]))
        series.append(jnp.where(first, other[half], own[half]))
    ends = jnp.zeros_like(series[0])
    begins = jnp.zeros_like(series[0])
    for k in range(3):
        ends = jnp.where(lane == k, pltpu.roll(series[k], k + 1, 1), ends)
        begin = series[k + 1] if k == 0 else pltpu.roll(series[k + 1], k, 1)
        begins = jnp.where(lane == k, begin, begins)
    edges = dot_full(begins, ends, ACROSS)
    cross = (cross_own_ref[...] + cross_other + edges) * scale
    cross_ref[...] = cross

    vectors = vec_ref[...]
    eigs = vectors.shape[0]
    on_diagonal = (
        lax.broadcasted_iota(jnp.int32, (eigs, eigs), 0)
        == lax.broadcasted_iota(jnp.int32, (eigs, eigs), 1)
    )
    values = jnp.sum(jnp.where(on_diagonal, val_ref[...][None, :], 0.0), axis=1, keepdims=True)

    top = jnp.max(jnp.sum(jnp.abs(square), axis=0, keepdims=True), axis=1, keepdims=True)
    bound_squared = top[0, 0]
    top = jnp.maximum(jnp.sqrt(top) * 1.001, 1.5)
    alpha = 2.0 / (top + 1.0)
    t1 = (top + 1.0) / (top - 1.0)
    t2 = 2.0 * t1 * t1 - 1.0
    i2 = 1.0 / t2
    c = 1.0 + i2
    r2 = c * (eye - (2.0 * alpha) * gram + (alpha * alpha) * square) - i2 * eye
    x2 = (c * alpha) * (2.0 * eye - alpha * gram)
    r_ref[...] = r2
    x_ref[...] = x2

    def doubled_x(t, x, rp):
        return (1.0 + 1.0 / t) * (x + dot3(pieces(x), rp))

    def doubled_r(t, rp):
        return (1.0 + 1.0 / t) * dot3(rp, rp) - (1.0 / t) * eye

    def answer(t, x, cross, gram):
        xp = pieces(x)
        guess = dot3(pieces(cross), xp)
        seen = dot_full(vectors, guess, ACROSS)
        mixed = dot3(pieces(vectors), xp, ACROSS)
        rest = pieces(cross - dot_full(guess, gram))
        last = 1.0 + 1.0 / (2.0 * t * t - 1.0)
        op_ref[...] = last * (guess + dot3(rest, xp))
        seen_ref[...] = last * (seen + dot3(pieces(mixed), rest, ACROSS))

    rp2 = pieces(r2)
    t4 = 2.0 * t2 * t2 - 1.0
    t8 = 2.0 * t4 * t4 - 1.0
    x4 = doubled_x(t4, x2, rp2)
    x8 = doubled_x(t8, x4, pieces(doubled_r(t4, rp2)))
    answer(t8, x8, cross, gram)

    small, fast = (bound_for(2) / 1.001) ** 2, LARGEST_FAST**2
    doublings = jnp.int32(1)
    for k in range(2, 8):
        doublings += (bound_squared > (bound_for(k) / 1.001) ** 2).astype(jnp.int32)

    @pl.when(jnp.logical_and(bound_squared > small, bound_squared <= fast))
    def _():
        def double(_, t):
            t = 2.0 * t * t - 1.0
            rp = pieces(r_ref[...])
            x_ref[...] = doubled_x(t, x_ref[...], rp)
            r_ref[...] = doubled_r(t, rp)
            return t

        t = lax.fori_loop(0, doublings, double, t2)
        t = 2.0 * t * t - 1.0
        x_ref[...] = doubled_x(t, x_ref[...], pieces(r_ref[...]))
        answer(t, x_ref[...], cross_ref[...], gram_ref[...])

        def again(_, carry):
            guess = op_ref[...]
            rest = cross_ref[...] - dot_full(guess, gram_ref[...])
            op_ref[...] = guess + dot3(pieces(rest), pieces(x_ref[...]))
            return carry

        lax.fori_loop(0, jnp.where(bound_squared > 32.0**2, 3, 0), again, 0)

    @pl.when(bound_squared > fast)
    def _():
        work[:, :width] = gram_ref[...]
        work[:, width:] = cross_ref[...].T
        eliminate(gram_ref, work, width)
        op_ref[...] = work[:, width:].T

    out = pltpu.make_async_copy(op_ref, op_out, sems.at[0])
    out.start()

    @pl.when(bound_squared > 32.0**2)
    def _():
        seen_ref[...] = dot_full(vectors, op_ref[...], ACROSS)

    residual = seen_ref[...] - values * vectors
    res_ref[...] = residual
    res = pltpu.make_async_copy(res_ref, res_out, sems.at[1])
    res.start()
    sums = jnp.sum(residual * residual, axis=1, keepdims=True)
    sums = jnp.sum(jnp.where(on_diagonal, sums, 0.0), axis=0)
    norm_ref[...] = jnp.sqrt(sums + 1e-06)
    norm = pltpu.make_async_copy(norm_ref, norm_out, sems.at[2])
    norm.start()
    out.wait()
    res.wait()
    norm.wait()


def solve(own, other, gram_own, cross_own, vectors, values, core_of=core_index):
    eigs, width = vectors.shape
    vmem = pl.BlockSpec(memory_space=pltpu.VMEM)
    hbm = pl.BlockSpec(memory_space=pltpu.HBM)
    square = pltpu.VMEM((width, width), jnp.float32)
    return pl.pallas_call(
        functools.partial(solve_kernel, core_of),
        out_shape=(
            jax.ShapeDtypeStruct((width, width), jnp.float32),
            jax.ShapeDtypeStruct((eigs, width), jnp.float32),
            jax.ShapeDtypeStruct((eigs,), jnp.float32),
        ),
        in_specs=[vmem] * 6,
        out_specs=(hbm, hbm, hbm),
        scratch_shapes=[square] * 5
        + [
            pltpu.VMEM((width, 2 * width), jnp.float32),
            pltpu.VMEM((eigs, width), jnp.float32),
            pltpu.VMEM((eigs, width), jnp.float32),
            pltpu.VMEM((eigs,), jnp.float32),
            pltpu.SemaphoreType.DMA((3,)),
        ],
        compiler_params=pltpu.CompilerParams(vmem_limit_bytes=16 * 2**20),
        name="solve",
    )(*map(near, (own, other, gram_own, cross_own, vectors, values)))


def project_kernel(chunk, modes_hbm, snaps_hbm, out, modes_vmem, snaps_vmem, total, mode_sem, snap_sem):
    steps = modes_hbm.shape[0] // chunk

    def copies(step):
        lines = pl.ds(step * chunk, chunk)
        return (
            pltpu.make_async_copy(modes_hbm.at[lines], modes_vmem.at[lines], mode_sem.at[step]),
            pltpu.make_async_copy(snaps_hbm.at[lines], snaps_vmem.at[lines], snap_sem.at[step]),
        )

    for step in range(steps):
        for copy in copies(step):
            copy.start()
    total[...] = jnp.zeros_like(total)

    def add(step, carry):
        for copy in copies(step):
            copy.wait()
        lines = pl.ds(pl.multiple_of(step * chunk, chunk), chunk)
        total[...] += lax.dot_general(
            snaps_vmem[lines, :],
            modes_vmem[lines, :],
            (((0,), (0,)), ((), ())),
            preferred_element_type=jnp.float32,
        )
        return carry

    lax.fori_loop(0, steps, add, 0)
    out[...] = total[...].T


def project(modes, snapshots, chunk=2048):
    width, cols = modes.shape[1], snapshots.shape[1]
    steps = modes.shape[0] // chunk
    far = functools.partial(pltpu.with_memory_space_constraint, memory_space=pltpu.HBM)
    return pl.pallas_call(
        functools.partial(project_kernel, chunk),
        out_shape=jax.ShapeDtypeStruct((width, cols), jnp.float32),
        in_specs=[pl.BlockSpec(memory_space=pltpu.HBM)] * 2,
        out_specs=pl.BlockSpec(memory_space=pltpu.VMEM),
        scratch_shapes=[
            pltpu.VMEM(modes.shape, modes.dtype),
            pltpu.VMEM(snapshots.shape, snapshots.dtype),
            pltpu.VMEM((cols, width), jnp.float32),
            pltpu.SemaphoreType.DMA((steps,)),
            pltpu.SemaphoreType.DMA((steps,)),
        ],
        compiler_params=pltpu.CompilerParams(vmem_limit_bytes=40 * 2**20),
        name="project",
    )(far(modes), far(snapshots))


def joint_groups():
    rows, halves = 32, 2
    return [[r * 4 + 2 * half + core for r in range(rows) for half in range(halves)] for core in range(2)]


def body(snapshots, modes, eig_vectors, eig_values):
    width = modes.shape[1]
    block_cols = snapshots.shape[1]
    rows = lax.axis_size("rows")
    partial_value = project(modes, snapshots)
    lines = width // rows
    arrived = lax.all_to_all(
        partial_value.reshape(rows, lines, block_cols), "rows", 0, 0, tiled=True
    )
    own_lines = jnp.sum(arrived, axis=0)
    axes = ("rows", "tm")
    gathered = lax.all_to_all(
        jnp.broadcast_to(own_lines[None], (2 * rows, lines, block_cols)),
        axes,
        0,
        0,
        tiled=True,
        axis_index_groups=joint_groups(),
    )
    swap = [(i, i ^ 1) for i in range(4 * rows)]
    other = lax.ppermute(gathered, axes, swap)
    shape = (rows, 2, lines, block_cols)
    own, other = gathered.reshape(shape), other.reshape(shape)
    gram_own, cross_own = own_sums(own, width)
    return solve(own, other, gram_own, cross_own, eig_vectors, eig_values)


def solution(mesh):
    return jax.shard_map(
        body,
        mesh=mesh,
        in_specs=(P("rows", "tm"), P("rows", None), P(), P()),
        out_specs=(P(), P(), P()),
        check_vma=False,
    )
```

```python
import functools
import math

import jax
import jax.numpy as jnp
from jax import lax
from jax.experimental import pallas as pl
from jax.experimental.pallas import tpu as pltpu
from jax.sharding import PartitionSpec as P

LARGEST_FAST = 2048.0
RESIDUAL_FLOOR = 224.0
PLANES = 2
PLAIN = ((1,), (0,))
ACROSS = ((1,), (1,))


def pieces(array):
    high = array.astype(jnp.bfloat16)
    low = (array - high.astype(jnp.float32)).astype(jnp.bfloat16)
    return high, low


def dot3(left, right, contract=PLAIN):
    left_high, left_low = left
    right_high, right_low = right

    def mm(a, b):
        return lax.dot_general(a, b, (contract, ((), ())), preferred_element_type=jnp.float32)

    return mm(left_high, right_high) + (mm(left_high, right_low) + mm(left_low, right_high))


def dot_full(left, right, contract=PLAIN):
    return lax.dot_general(
        left,
        right,
        (contract, ((), ())),
        precision=lax.Precision.HIGHEST,
        preferred_element_type=jnp.float32,
    )


def bound_for(doublings):
    t = RESIDUAL_FLOOR
    for _ in range(doublings + 1):
        t = math.sqrt((t + 1.0) / 2.0)
    return (t + 1.0) / (t - 1.0)


def eliminate(gram_ref, work, width):
    lanes = lax.broadcasted_iota(jnp.int32, (1, 2 * width), 1)
    lines = lax.broadcasted_iota(jnp.int32, (width, 1), 0)

    def step(k, carry):
        row = work[pl.ds(k, 1), :]
        here = (lanes == k).astype(jnp.float32)
        pivot = jnp.sum(row * here, axis=1, keepdims=True)
        row = row / pivot
        column = jnp.sum(work[...] * here, axis=1, keepdims=True)
        on_line = lines == k
        work[...] = jnp.where(on_line, row, work[...] - column * row)
        return carry

    lax.fori_loop(0, width, step, 0)


def core_index():
    return lax.axis_index("tm") & 1


def block_of(ref, half):
    return ref[:, half].reshape(-1, ref.shape[-1])


def half_sums(blocks, drop_last):
    cols = blocks[0].shape[1]
    column = lax.broadcasted_iota(jnp.int32, (1, cols), 1)
    inner = column < cols - 1
    leads = jnp.concatenate(
        [blocks[0], jnp.where(jnp.logical_or(inner, jnp.logical_not(drop_last)), blocks[1], 0.0)],
        axis=1,
    )
    starts = jnp.concatenate([jnp.where(inner, block, 0.0) for block in blocks], axis=1)
    nexts = jnp.concatenate([pltpu.roll(block, cols - 1, 1) for block in blocks], axis=1)
    gram = dot_full(leads, leads, ACROSS)
    cross = dot_full(nexts, starts, ACROSS)
    return gram, cross


def own_kernel(core_of, own_ref, gram_ref, cross_ref):
    blocks = [block_of(own_ref, 0), block_of(own_ref, 1)]
    gram, cross = half_sums(blocks, core_of() == 1)
    gram_ref[...] = gram
    cross_ref[...] = cross


def near(array):
    return pltpu.with_memory_space_constraint(array, pltpu.VMEM)


def own_sums(own, width, core_of=core_index):
    vmem = pl.BlockSpec(memory_space=pltpu.VMEM)
    square = jax.ShapeDtypeStruct((width, width), jnp.float32)
    return pl.pallas_call(
        functools.partial(own_kernel, core_of),
        out_shape=(square, square),
        in_specs=[vmem],
        out_specs=(vmem, vmem),
        compiler_params=pltpu.CompilerParams(vmem_limit_bytes=16 * 2**20),
        cost_estimate=pl.CostEstimate(
            flops=24 * width**3, bytes_accessed=12 * width * width, transcendentals=0
        ),
        name="own_sums",
    )(near(own))


def solve_kernel(core_of, own_ref, other_ref, gram_own_ref, cross_own_ref, vec_ref, val_ref,
                 op_out, res_out, norm_out,
                 gram_ref, cross_ref, r_ref, x_ref, op_ref, work, seen_ref, res_ref, norm_ref, sems):
    width = gram_ref.shape[0]
    core = core_of()
    first = core == 0
    own = [block_of(own_ref, half) for half in range(2)]
    other = [block_of(other_ref, half) for half in range(2)]
    cols = own[0].shape[1]
    scale = 1.0 / (4 * cols - 1)
    eye = (
        lax.broadcasted_iota(jnp.int32, (width, width), 0)
        == lax.broadcasted_iota(jnp.int32, (width, width), 1)
    ).astype(jnp.float32)
    gram_other, cross_other = half_sums(other, first)
    gram = (gram_own_ref[...] + gram_other) * scale + eye
    gram_ref[...] = gram
    gram_pieces = pieces(gram)
    square = dot3(gram_pieces, gram_pieces)

    lane = lax.broadcasted_iota(jnp.int32, (1, cols), 1)
    series = []
    for half in range(2):
        series.append(jnp.where(first, own[half], other[half]))
        series.append(jnp.where(first, other[half], own[half]))
    ends = jnp.zeros_like(series[0])
    begins = jnp.zeros_like(series[0])
    for k in range(3):
        ends = jnp.where(lane == k, pltpu.roll(series[k], k + 1, 1), ends)
        begin = series[k + 1] if k == 0 else pltpu.roll(series[k + 1], k, 1)
        begins = jnp.where(lane == k, begin, begins)
    edges = dot_full(begins, ends, ACROSS)
    cross_ref[...] = (cross_own_ref[...] + cross_other + edges) * scale

    vectors = vec_ref[...]
    eigs = vectors.shape[0]
    on_diagonal = (
        lax.broadcasted_iota(jnp.int32, (eigs, eigs), 0)
        == lax.broadcasted_iota(jnp.int32, (eigs, eigs), 1)
    )
    values = jnp.sum(jnp.where(on_diagonal, val_ref[...][None, :], 0.0), axis=1, keepdims=True)

    top = jnp.max(jnp.sum(jnp.abs(square), axis=0, keepdims=True), axis=1, keepdims=True)
    bound_squared = top[0, 0]
    top = jnp.maximum(jnp.sqrt(top) * 1.001, 1.5)
    doublings = jnp.int32(0)
    for k in range(1, 8):
        doublings += (bound_squared > (bound_for(k) / 1.001) ** 2).astype(jnp.int32)

    @pl.when(bound_squared <= LARGEST_FAST**2)
    def _():
        alpha = 2.0 / (top + 1.0)
        t1 = (top + 1.0) / (top - 1.0)
        t2 = 2.0 * t1 * t1 - 1.0
        i2 = 1.0 / t2
        c = 1.0 + i2
        r_ref[...] = c * (eye - (2.0 * alpha) * gram_ref[...] + (alpha * alpha) * square) - i2 * eye
        x_ref[...] = (c * alpha) * (2.0 * eye - alpha * gram_ref[...])

        def double(_, t):
            t = 2.0 * t * t - 1.0
            it = 1.0 / t
            x = x_ref[...]
            rp = pieces(r_ref[...])
            x_ref[...] = (1.0 + it) * (x + dot3(pieces(x), rp))
            r_ref[...] = (1.0 + it) * dot3(rp, rp) - it * eye
            return t

        t = lax.fori_loop(0, doublings, double, t2)
        t = 2.0 * t * t - 1.0
        x = x_ref[...]
        x = (1.0 + 1.0 / t) * (x + dot3(pieces(x), pieces(r_ref[...])))
        x_ref[...] = x
        xp = pieces(x)

        guess = dot3(pieces(cross_ref[...]), xp)
        seen = dot_full(vectors, guess, ACROSS)
        mixed = dot3(pieces(vectors), xp, ACROSS)
        rest = pieces(cross_ref[...] - dot_full(guess, gram_ref[...]))
        last = 1.0 + 1.0 / (2.0 * t * t - 1.0)
        op_ref[...] = last * (guess + dot3(rest, xp))
        seen_ref[...] = last * (seen + dot3(pieces(mixed), rest, ACROSS))

    @pl.when(jnp.logical_and(bound_squared > 32.0**2, bound_squared <= LARGEST_FAST**2))
    def _():
        def again(_, carry):
            guess = op_ref[...]
            rest = cross_ref[...] - dot_full(guess, gram_ref[...])
            op_ref[...] = guess + dot3(pieces(rest), pieces(x_ref[...]))
            return carry

        lax.fori_loop(0, 3, again, 0)

    @pl.when(bound_squared > LARGEST_FAST**2)
    def _():
        work[:, :width] = gram_ref[...]
        work[:, width:] = cross_ref[...].T
        eliminate(gram_ref, work, width)
        op_ref[...] = work[:, width:].T

    out = pltpu.make_async_copy(op_ref, op_out, sems.at[0])
    out.start()

    @pl.when(bound_squared > 32.0**2)
    def _():
        seen_ref[...] = dot_full(vectors, op_ref[...], ACROSS)

    residual = seen_ref[...] - values * vectors
    res_ref[...] = residual
    res = pltpu.make_async_copy(res_ref, res_out, sems.at[1])
    res.start()
    sums = jnp.sum(residual * residual, axis=1, keepdims=True)
    sums = jnp.sum(jnp.where(on_diagonal, sums, 0.0), axis=0)
    norm_ref[...] = jnp.sqrt(sums + 1e-06)
    norm = pltpu.make_async_copy(norm_ref, norm_out, sems.at[2])
    norm.start()
    out.wait()
    res.wait()
    norm.wait()


def solve(own, other, gram_own, cross_own, vectors, values, core_of=core_index):
    eigs, width = vectors.shape
    vmem = pl.BlockSpec(memory_space=pltpu.VMEM)
    hbm = pl.BlockSpec(memory_space=pltpu.HBM)
    square = pltpu.VMEM((width, width), jnp.float32)
    return pl.pallas_call(
        functools.partial(solve_kernel, core_of),
        out_shape=(
            jax.ShapeDtypeStruct((width, width), jnp.float32),
            jax.ShapeDtypeStruct((eigs, width), jnp.float32),
            jax.ShapeDtypeStruct((eigs,), jnp.float32),
        ),
        in_specs=[vmem] * 6,
        out_specs=(hbm, hbm, hbm),
        scratch_shapes=[square] * 5
        + [
            pltpu.VMEM((width, 2 * width), jnp.float32),
            pltpu.VMEM((eigs, width), jnp.float32),
            pltpu.VMEM((eigs, width), jnp.float32),
            pltpu.VMEM((eigs,), jnp.float32),
            pltpu.SemaphoreType.DMA((3,)),
        ],
        compiler_params=pltpu.CompilerParams(vmem_limit_bytes=16 * 2**20),
        name="solve",
    )(*map(near, (own, other, gram_own, cross_own, vectors, values)))


def project_kernel(chunk, modes_hbm, snaps_hbm, out, modes_vmem, snaps_vmem, total, mode_sem, snap_sem):
    steps = modes_hbm.shape[0] // chunk

    def copies(step):
        lines = pl.ds(step * chunk, chunk)
        return (
            pltpu.make_async_copy(modes_hbm.at[lines], modes_vmem.at[lines], mode_sem.at[step]),
            pltpu.make_async_copy(snaps_hbm.at[lines], snaps_vmem.at[lines], snap_sem.at[step]),
        )

    for step in range(steps):
        for copy in copies(step):
            copy.start()
    total[...] = jnp.zeros_like(total)

    def add(step, carry):
        for copy in copies(step):
            copy.wait()
        lines = pl.ds(pl.multiple_of(step * chunk, chunk), chunk)
        total[...] += lax.dot_general(
            snaps_vmem[lines, :],
            modes_vmem[lines, :],
            (((0,), (0,)), ((), ())),
            preferred_element_type=jnp.float32,
        )
        return carry

    lax.fori_loop(0, steps, add, 0)
    sums = total[...].T
    for copy in range(PLANES):
        out[copy] = sums


def project(modes, snapshots, chunk=2048):
    width, cols = modes.shape[1], snapshots.shape[1]
    steps = modes.shape[0] // chunk
    far = functools.partial(pltpu.with_memory_space_constraint, memory_space=pltpu.HBM)
    return pl.pallas_call(
        functools.partial(project_kernel, chunk),
        out_shape=jax.ShapeDtypeStruct((PLANES, width, cols), jnp.float32),
        in_specs=[pl.BlockSpec(memory_space=pltpu.HBM)] * 2,
        out_specs=pl.BlockSpec(memory_space=pltpu.VMEM),
        scratch_shapes=[
            pltpu.VMEM(modes.shape, modes.dtype),
            pltpu.VMEM(snapshots.shape, snapshots.dtype),
            pltpu.VMEM((cols, width), jnp.float32),
            pltpu.SemaphoreType.DMA((steps,)),
            pltpu.SemaphoreType.DMA((steps,)),
        ],
        compiler_params=pltpu.CompilerParams(vmem_limit_bytes=40 * 2**20),
        name="project",
    )(far(modes), far(snapshots))


def gather_groups(rows, times):
    plane = rows // PLANES
    return [
        [(high * plane + r) * times + 2 * low + core for r in range(plane) for low in range(2)]
        for high in range(PLANES)
        for core in range(2)
    ]


def body(snapshots, modes, eig_vectors, eig_values):
    width = modes.shape[1]
    block_cols = snapshots.shape[1]
    rows, times = lax.axis_size("rows"), lax.axis_size("tm")
    plane = rows // PLANES
    lines = width // plane
    partial_value = project(modes, snapshots)
    arrived = lax.all_to_all(
        partial_value.reshape(rows, lines, block_cols), "rows", 0, 0, tiled=True
    )
    own_lines = jnp.sum(arrived, axis=0)
    axes = ("rows", "tm")
    gathered = lax.all_to_all(
        jnp.broadcast_to(own_lines[None], (2 * plane, lines, block_cols)),
        axes,
        0,
        0,
        tiled=True,
        axis_index_groups=gather_groups(rows, times),
    )
    other = lax.ppermute(gathered, axes, [(i, i ^ 1) for i in range(times * rows)])
    shape = (plane, 2, lines, block_cols)
    own, other = gathered.reshape(shape), other.reshape(shape)
    gram_own, cross_own = own_sums(own, width)
    return solve(own, other, gram_own, cross_own, eig_vectors, eig_values)


def solution(mesh):
    return jax.shard_map(
        body,
        mesh=mesh,
        in_specs=(P("rows", "tm"), P("rows", None), P(), P()),
        out_specs=(P(), P(), P()),
        check_vma=False,
    )
```

```python
import functools
import math

import jax
import jax.numpy as jnp
from jax import lax
from jax.experimental import pallas as pl
from jax.experimental.pallas import tpu as pltpu
from jax.sharding import PartitionSpec as P

LARGEST_FAST = 2048.0
RESIDUAL_FLOOR = 224.0
PLAIN = ((1,), (0,))
ACROSS = ((1,), (1,))


def pieces(array):
    high = array.astype(jnp.bfloat16)
    low = (array - high.astype(jnp.float32)).astype(jnp.bfloat16)
    return high, low


def dot3(left, right, contract=PLAIN):
    left_high, left_low = left
    right_high, right_low = right

    def mm(a, b):
        return lax.dot_general(a, b, (contract, ((), ())), preferred_element_type=jnp.float32)

    return mm(left_high, right_high) + (mm(left_high, right_low) + mm(left_low, right_high))


def dot_full(left, right, contract=PLAIN):
    return lax.dot_general(
        left,
        right,
        (contract, ((), ())),
        precision=lax.Precision.HIGHEST,
        preferred_element_type=jnp.float32,
    )


def bound_for(doublings):
    t = RESIDUAL_FLOOR
    for _ in range(doublings + 1):
        t = math.sqrt((t + 1.0) / 2.0)
    return (t + 1.0) / (t - 1.0)


def eliminate(gram_ref, work, width):
    lanes = lax.broadcasted_iota(jnp.int32, (1, 2 * width), 1)
    lines = lax.broadcasted_iota(jnp.int32, (width, 1), 0)

    def step(k, carry):
        row = work[pl.ds(k, 1), :]
        here = (lanes == k).astype(jnp.float32)
        pivot = jnp.sum(row * here, axis=1, keepdims=True)
        row = row / pivot
        column = jnp.sum(work[...] * here, axis=1, keepdims=True)
        on_line = lines == k
        work[...] = jnp.where(on_line, row, work[...] - column * row)
        return carry

    lax.fori_loop(0, width, step, 0)


def core_index():
    return lax.axis_index("tm") & 1


def block_of(ref, half):
    return ref[:, half].reshape(-1, ref.shape[-1])


def half_sums(blocks, drop_last):
    cols = blocks[0].shape[1]
    column = lax.broadcasted_iota(jnp.int32, (1, cols), 1)
    inner = column < cols - 1
    leads = jnp.concatenate(
        [blocks[0], jnp.where(jnp.logical_or(inner, jnp.logical_not(drop_last)), blocks[1], 0.0)],
        axis=1,
    )
    starts = jnp.concatenate([jnp.where(inner, block, 0.0) for block in blocks], axis=1)
    nexts = jnp.concatenate([pltpu.roll(block, cols - 1, 1) for block in blocks], axis=1)
    gram = dot_full(leads, leads, ACROSS)
    cross = dot_full(nexts, starts, ACROSS)
    return gram, cross


def own_kernel(core_of, own_ref, gram_ref, cross_ref):
    blocks = [block_of(own_ref, 0), block_of(own_ref, 1)]
    gram, cross = half_sums(blocks, core_of() == 1)
    gram_ref[...] = gram
    cross_ref[...] = cross


def near(array):
    return pltpu.with_memory_space_constraint(array, pltpu.VMEM)


def own_sums(own, width, core_of=core_index):
    vmem = pl.BlockSpec(memory_space=pltpu.VMEM)
    square = jax.ShapeDtypeStruct((width, width), jnp.float32)
    return pl.pallas_call(
        functools.partial(own_kernel, core_of),
        out_shape=(square, square),
        in_specs=[vmem],
        out_specs=(vmem, vmem),
        compiler_params=pltpu.CompilerParams(vmem_limit_bytes=16 * 2**20),
        cost_estimate=pl.CostEstimate(
            flops=24 * width**3, bytes_accessed=12 * width * width, transcendentals=0
        ),
        name="own_sums",
    )(near(own))


def solve_kernel(core_of, own_ref, other_ref, gram_own_ref, cross_own_ref, vec_ref, val_ref,
                 op_out, res_out, norm_out,
                 gram_ref, cross_ref, r_ref, x_ref, op_ref, work, seen_ref, res_ref, norm_ref, sems):
    width = gram_ref.shape[0]
    core = core_of()
    first = core == 0
    own = [block_of(own_ref, half) for half in range(2)]
    other = [block_of(other_ref, half) for half in range(2)]
    cols = own[0].shape[1]
    scale = 1.0 / (4 * cols - 1)
    eye = (
        lax.broadcasted_iota(jnp.int32, (width, width), 0)
        == lax.broadcasted_iota(jnp.int32, (width, width), 1)
    ).astype(jnp.float32)
    gram_other, cross_other = half_sums(other, first)
    gram = (gram_own_ref[...] + gram_other) * scale + eye
    gram_ref[...] = gram
    gram_pieces = pieces(gram)
    square = dot3(gram_pieces, gram_pieces)

    lane = lax.broadcasted_iota(jnp.int32, (1, cols), 1)
    series = []
    for half in range(2):
        series.append(jnp.where(first, own[half], other[half]))
        series.append(jnp.where(first, other[half], own[half]))
    ends = jnp.zeros_like(series[0])
    begins = jnp.zeros_like(series[0])
    for k in range(3):
        ends = jnp.where(lane == k, pltpu.roll(series[k], k + 1, 1), ends)
        begin = series[k + 1] if k == 0 else pltpu.roll(series[k + 1], k, 1)
        begins = jnp.where(lane == k, begin, begins)
    edges = dot_full(begins, ends, ACROSS)
    cross_ref[...] = (cross_own_ref[...] + cross_other + edges) * scale

    vectors = vec_ref[...]
    eigs = vectors.shape[0]
    on_diagonal = (
        lax.broadcasted_iota(jnp.int32, (eigs, eigs), 0)
        == lax.broadcasted_iota(jnp.int32, (eigs, eigs), 1)
    )
    values = jnp.sum(jnp.where(on_diagonal, val_ref[...][None, :], 0.0), axis=1, keepdims=True)

    top = jnp.max(jnp.sum(jnp.abs(square), axis=0, keepdims=True), axis=1, keepdims=True)
    bound_squared = top[0, 0]
    top = jnp.maximum(jnp.sqrt(top) * 1.001, 1.5)
    doublings = jnp.int32(0)
    for k in range(1, 8):
        doublings += (bound_squared > (bound_for(k) / 1.001) ** 2).astype(jnp.int32)

    @pl.when(bound_squared <= LARGEST_FAST**2)
    def _():
        alpha = 2.0 / (top + 1.0)
        t1 = (top + 1.0) / (top - 1.0)
        t2 = 2.0 * t1 * t1 - 1.0
        i2 = 1.0 / t2
        c = 1.0 + i2
        r_ref[...] = c * (eye - (2.0 * alpha) * gram_ref[...] + (alpha * alpha) * square) - i2 * eye
        x_ref[...] = (c * alpha) * (2.0 * eye - alpha * gram_ref[...])

        def double(_, t):
            t = 2.0 * t * t - 1.0
            it = 1.0 / t
            x = x_ref[...]
            rp = pieces(r_ref[...])
            x_ref[...] = (1.0 + it) * (x + dot3(pieces(x), rp))
            r_ref[...] = (1.0 + it) * dot3(rp, rp) - it * eye
            return t

        t = lax.fori_loop(0, doublings, double, t2)
        t = 2.0 * t * t - 1.0
        x = x_ref[...]
        x = (1.0 + 1.0 / t) * (x + dot3(pieces(x), pieces(r_ref[...])))
        x_ref[...] = x
        xp = pieces(x)

        guess = dot3(pieces(cross_ref[...]), xp)
        seen = dot_full(vectors, guess, ACROSS)
        mixed = dot3(pieces(vectors), xp, ACROSS)
        rest = pieces(cross_ref[...] - dot_full(guess, gram_ref[...]))
        last = 1.0 + 1.0 / (2.0 * t * t - 1.0)
        op_ref[...] = last * (guess + dot3(rest, xp))
        seen_ref[...] = last * (seen + dot3(pieces(mixed), rest, ACROSS))

    @pl.when(jnp.logical_and(bound_squared > 32.0**2, bound_squared <= LARGEST_FAST**2))
    def _():
        def again(_, carry):
            guess = op_ref[...]
            rest = cross_ref[...] - dot_full(guess, gram_ref[...])
            op_ref[...] = guess + dot3(pieces(rest), pieces(x_ref[...]))
            return carry

        lax.fori_loop(0, 3, again, 0)

    @pl.when(bound_squared > LARGEST_FAST**2)
    def _():
        work[:, :width] = gram_ref[...]
        work[:, width:] = cross_ref[...].T
        eliminate(gram_ref, work, width)
        op_ref[...] = work[:, width:].T

    out = pltpu.make_async_copy(op_ref, op_out, sems.at[0])
    out.start()

    @pl.when(bound_squared > 32.0**2)
    def _():
        seen_ref[...] = dot_full(vectors, op_ref[...], ACROSS)

    residual = seen_ref[...] - values * vectors
    res_ref[...] = residual
    res = pltpu.make_async_copy(res_ref, res_out, sems.at[1])
    res.start()
    sums = jnp.sum(residual * residual, axis=1, keepdims=True)
    sums = jnp.sum(jnp.where(on_diagonal, sums, 0.0), axis=0)
    norm_ref[...] = jnp.sqrt(sums + 1e-06)
    norm = pltpu.make_async_copy(norm_ref, norm_out, sems.at[2])
    norm.start()
    out.wait()
    res.wait()
    norm.wait()


def solve(own, other, gram_own, cross_own, vectors, values, core_of=core_index):
    eigs, width = vectors.shape
    vmem = pl.BlockSpec(memory_space=pltpu.VMEM)
    hbm = pl.BlockSpec(memory_space=pltpu.HBM)
    square = pltpu.VMEM((width, width), jnp.float32)
    return pl.pallas_call(
        functools.partial(solve_kernel, core_of),
        out_shape=(
            jax.ShapeDtypeStruct((width, width), jnp.float32),
            jax.ShapeDtypeStruct((eigs, width), jnp.float32),
            jax.ShapeDtypeStruct((eigs,), jnp.float32),
        ),
        in_specs=[vmem] * 6,
        out_specs=(hbm, hbm, hbm),
        scratch_shapes=[square] * 5
        + [
            pltpu.VMEM((width, 2 * width), jnp.float32),
            pltpu.VMEM((eigs, width), jnp.float32),
            pltpu.VMEM((eigs, width), jnp.float32),
            pltpu.VMEM((eigs,), jnp.float32),
            pltpu.SemaphoreType.DMA((3,)),
        ],
        compiler_params=pltpu.CompilerParams(vmem_limit_bytes=16 * 2**20),
        name="solve",
    )(*map(near, (own, other, gram_own, cross_own, vectors, values)))


def project_kernel(chunk, owner, lines, modes_hbm, snaps_hbm, out, modes_vmem, snaps_vmem, total, mode_sem, snap_sem):
    steps = modes_hbm.shape[0] // chunk

    def copies(step):
        lines = pl.ds(step * chunk, chunk)
        return (
            pltpu.make_async_copy(modes_hbm.at[lines], modes_vmem.at[lines], mode_sem.at[step]),
            pltpu.make_async_copy(snaps_hbm.at[lines], snaps_vmem.at[lines], snap_sem.at[step]),
        )

    for step in range(steps):
        for copy in copies(step):
            copy.start()
    total[...] = jnp.zeros_like(total)

    def add(step, carry):
        for copy in copies(step):
            copy.wait()
        lines = pl.ds(pl.multiple_of(step * chunk, chunk), chunk)
        total[...] += lax.dot_general(
            snaps_vmem[lines, :],
            modes_vmem[lines, :],
            (((0,), (0,)), ((), ())),
            preferred_element_type=jnp.float32,
        )
        return carry

    lax.fori_loop(0, steps, add, 0)
    sums = total[...].T
    for place, block in enumerate(owner):
        out[place] = sums[block * lines : (block + 1) * lines]


def project(modes, snapshots, owner, lines, chunk=2048):
    width, cols = modes.shape[1], snapshots.shape[1]
    steps = modes.shape[0] // chunk
    far = functools.partial(pltpu.with_memory_space_constraint, memory_space=pltpu.HBM)
    return pl.pallas_call(
        functools.partial(project_kernel, chunk, owner, lines),
        out_shape=jax.ShapeDtypeStruct((len(owner), lines, cols), jnp.float32),
        in_specs=[pl.BlockSpec(memory_space=pltpu.HBM)] * 2,
        out_specs=pl.BlockSpec(memory_space=pltpu.VMEM),
        scratch_shapes=[
            pltpu.VMEM(modes.shape, modes.dtype),
            pltpu.VMEM(snapshots.shape, snapshots.dtype),
            pltpu.VMEM((cols, width), jnp.float32),
            pltpu.SemaphoreType.DMA((steps,)),
            pltpu.SemaphoreType.DMA((steps,)),
        ],
        compiler_params=pltpu.CompilerParams(vmem_limit_bytes=40 * 2**20),
        name="project",
    )(far(modes), far(snapshots))


DIMS = "YZzXx"
FIRST = 'ZzXx'
COPIES = 'X'


def plan(rows, times):
    kept = [d for d in DIMS if d in FIRST and d not in COPIES]
    partial = [d for d in DIMS if d not in FIRST]
    places = [dict(zip(DIMS, ((r >> (4 - k)) & 1 for k in range(5)))) for r in range(rows)]

    def packed(place, dims):
        return sum(place[d] << k for k, d in enumerate(reversed(dims)))

    owner = [packed(place, kept) for place in places]
    first, second = {}, {}
    for r, place in enumerate(places):
        first.setdefault(packed(place, partial), []).append(r)
        second.setdefault(packed(place, list(COPIES)), []).append((packed(place, partial + kept), r))
    members = [first[k] for k in sorted(first)]
    gathers = [
        [r * times + 2 * low + core for _, r in sorted(second[k]) for low in range(2)]
        for k in sorted(second)
        for core in range(2)
    ]
    return [owner[r] for r in members[0]], members, gathers, 2 ** len(kept), 2 ** len(partial)


def body(snapshots, modes, eig_vectors, eig_values):
    width = modes.shape[1]
    block_cols = snapshots.shape[1]
    rows, times = lax.axis_size("rows"), lax.axis_size("tm")
    owner, members, gathers, owners, parts = plan(rows, times)
    lines = width // owners
    sent = project(modes, snapshots, owner, lines)
    arrived = lax.all_to_all(sent, "rows", 0, 0, tiled=True, axis_index_groups=members)
    own_lines = jnp.sum(arrived, axis=0)
    axes = ("rows", "tm")
    gathered = lax.all_to_all(
        jnp.broadcast_to(own_lines[None], (2 * owners * parts, lines, block_cols)),
        axes,
        0,
        0,
        tiled=True,
        axis_index_groups=gathers,
    )
    if parts > 1:
        gathered = jnp.sum(gathered.reshape(parts, 2 * owners, lines, block_cols), axis=0)
    other = lax.ppermute(gathered, axes, [(i, i ^ 1) for i in range(times * rows)])
    shape = (owners, 2, lines, block_cols)
    own, other = gathered.reshape(shape), other.reshape(shape)
    gram_own, cross_own = own_sums(own, width)
    return solve(own, other, gram_own, cross_own, eig_vectors, eig_values)


def solution(mesh):
    return jax.shard_map(
        body,
        mesh=mesh,
        in_specs=(P("rows", "tm"), P("rows", None), P(), P()),
        out_specs=(P(), P(), P()),
        check_vma=False,
    )
```

```python
import functools
import math

import jax
import jax.numpy as jnp
from jax import lax
from jax.experimental import pallas as pl
from jax.experimental.pallas import tpu as pltpu
from jax.sharding import PartitionSpec as P

LARGEST_FAST = 2048.0
RESIDUAL_FLOOR = 224.0
PLAIN = ((1,), (0,))
ACROSS = ((1,), (1,))


def pieces(array):
    high = array.astype(jnp.bfloat16)
    low = (array - high.astype(jnp.float32)).astype(jnp.bfloat16)
    return high, low


def dot3(left, right, contract=PLAIN):
    left_high, left_low = left
    right_high, right_low = right

    def mm(a, b):
        return lax.dot_general(a, b, (contract, ((), ())), preferred_element_type=jnp.float32)

    return mm(left_high, right_high) + (mm(left_high, right_low) + mm(left_low, right_high))


def dot_full(left, right, contract=PLAIN):
    return lax.dot_general(
        left,
        right,
        (contract, ((), ())),
        precision=lax.Precision.HIGHEST,
        preferred_element_type=jnp.float32,
    )


def bound_for(doublings):
    t = RESIDUAL_FLOOR
    for _ in range(doublings + 1):
        t = math.sqrt((t + 1.0) / 2.0)
    return (t + 1.0) / (t - 1.0)


def eliminate(gram_ref, work, width):
    lanes = lax.broadcasted_iota(jnp.int32, (1, 2 * width), 1)
    lines = lax.broadcasted_iota(jnp.int32, (width, 1), 0)

    def step(k, carry):
        row = work[pl.ds(k, 1), :]
        here = (lanes == k).astype(jnp.float32)
        pivot = jnp.sum(row * here, axis=1, keepdims=True)
        row = row / pivot
        column = jnp.sum(work[...] * here, axis=1, keepdims=True)
        on_line = lines == k
        work[...] = jnp.where(on_line, row, work[...] - column * row)
        return carry

    lax.fori_loop(0, width, step, 0)


def core_index():
    return lax.axis_index("tm") & 1


def block_of(ref, half):
    return ref[:, half].reshape(-1, ref.shape[-1])


def half_sums(blocks, drop_last):
    cols = blocks[0].shape[1]
    column = lax.broadcasted_iota(jnp.int32, (1, cols), 1)
    inner = column < cols - 1
    leads = jnp.concatenate(
        [blocks[0], jnp.where(jnp.logical_or(inner, jnp.logical_not(drop_last)), blocks[1], 0.0)],
        axis=1,
    )
    starts = jnp.concatenate([jnp.where(inner, block, 0.0) for block in blocks], axis=1)
    nexts = jnp.concatenate([pltpu.roll(block, cols - 1, 1) for block in blocks], axis=1)
    gram = dot_full(leads, leads, ACROSS)
    cross = dot_full(nexts, starts, ACROSS)
    return gram, cross


def own_kernel(core_of, own_ref, gram_ref, cross_ref):
    blocks = [block_of(own_ref, 0), block_of(own_ref, 1)]
    gram, cross = half_sums(blocks, core_of() == 1)
    gram_ref[...] = gram
    cross_ref[...] = cross


def near(array):
    return pltpu.with_memory_space_constraint(array, pltpu.VMEM)


def own_sums(own, width, core_of=core_index):
    vmem = pl.BlockSpec(memory_space=pltpu.VMEM)
    square = jax.ShapeDtypeStruct((width, width), jnp.float32)
    return pl.pallas_call(
        functools.partial(own_kernel, core_of),
        out_shape=(square, square),
        in_specs=[vmem],
        out_specs=(vmem, vmem),
        compiler_params=pltpu.CompilerParams(vmem_limit_bytes=16 * 2**20),
        cost_estimate=pl.CostEstimate(
            flops=24 * width**3, bytes_accessed=12 * width * width, transcendentals=0
        ),
        name="own_sums",
    )(near(own))


def solve_kernel(core_of, own_ref, other_ref, gram_own_ref, cross_own_ref, vec_ref, val_ref,
                 op_out, res_out, norm_out,
                 gram_ref, cross_ref, r_ref, x_ref, op_ref, work, seen_ref, res_ref, norm_ref, sems):
    width = gram_ref.shape[0]
    core = core_of()
    first = core == 0
    own = [block_of(own_ref, half) for half in range(2)]
    other = [block_of(other_ref, half) for half in range(2)]
    cols = own[0].shape[1]
    scale = 1.0 / (4 * cols - 1)
    eye = (
        lax.broadcasted_iota(jnp.int32, (width, width), 0)
        == lax.broadcasted_iota(jnp.int32, (width, width), 1)
    ).astype(jnp.float32)
    gram_other, cross_other = half_sums(other, first)
    gram = (gram_own_ref[...] + gram_other) * scale + eye
    gram_ref[...] = gram
    gram_pieces = pieces(gram)
    square = dot3(gram_pieces, gram_pieces)

    lane = lax.broadcasted_iota(jnp.int32, (1, cols), 1)
    series = []
    for half in range(2):
        series.append(jnp.where(first, own[half], other[half]))
        series.append(jnp.where(first, other[half], own[half]))
    ends = jnp.zeros_like(series[0])
    begins = jnp.zeros_like(series[0])
    for k in range(3):
        ends = jnp.where(lane == k, pltpu.roll(series[k], k + 1, 1), ends)
        begin = series[k + 1] if k == 0 else pltpu.roll(series[k + 1], k, 1)
        begins = jnp.where(lane == k, begin, begins)
    edges = dot_full(begins, ends, ACROSS)
    cross_ref[...] = (cross_own_ref[...] + cross_other + edges) * scale

    vectors = vec_ref[...]
    eigs = vectors.shape[0]
    on_diagonal = (
        lax.broadcasted_iota(jnp.int32, (eigs, eigs), 0)
        == lax.broadcasted_iota(jnp.int32, (eigs, eigs), 1)
    )
    values = jnp.sum(jnp.where(on_diagonal, val_ref[...][None, :], 0.0), axis=1, keepdims=True)

    top = jnp.max(jnp.sum(jnp.abs(square), axis=0, keepdims=True), axis=1, keepdims=True)
    bound_squared = top[0, 0]
    top = jnp.maximum(jnp.sqrt(top) * 1.001, 1.5)
    doublings = jnp.int32(0)
    for k in range(1, 8):
        doublings += (bound_squared > (bound_for(k) / 1.001) ** 2).astype(jnp.int32)

    @pl.when(bound_squared <= LARGEST_FAST**2)
    def _():
        alpha = 2.0 / (top + 1.0)
        t1 = (top + 1.0) / (top - 1.0)
        t2 = 2.0 * t1 * t1 - 1.0
        i2 = 1.0 / t2
        c = 1.0 + i2
        r_ref[...] = c * (eye - (2.0 * alpha) * gram_ref[...] + (alpha * alpha) * square) - i2 * eye
        x_ref[...] = (c * alpha) * (2.0 * eye - alpha * gram_ref[...])

        def double(_, t):
            t = 2.0 * t * t - 1.0
            it = 1.0 / t
            x = x_ref[...]
            rp = pieces(r_ref[...])
            x_ref[...] = (1.0 + it) * (x + dot3(pieces(x), rp))
            r_ref[...] = (1.0 + it) * dot3(rp, rp) - it * eye
            return t

        t = lax.fori_loop(0, doublings, double, t2)
        t = 2.0 * t * t - 1.0
        x = x_ref[...]
        x = (1.0 + 1.0 / t) * (x + dot3(pieces(x), pieces(r_ref[...])))
        x_ref[...] = x
        xp = pieces(x)

        guess = dot3(pieces(cross_ref[...]), xp)
        seen = dot_full(vectors, guess, ACROSS)
        mixed = dot3(pieces(vectors), xp, ACROSS)
        rest = pieces(cross_ref[...] - dot_full(guess, gram_ref[...]))
        last = 1.0 + 1.0 / (2.0 * t * t - 1.0)
        op_ref[...] = last * (guess + dot3(rest, xp))
        seen_ref[...] = last * (seen + dot3(pieces(mixed), rest, ACROSS))

    @pl.when(jnp.logical_and(bound_squared > 32.0**2, bound_squared <= LARGEST_FAST**2))
    def _():
        def again(_, carry):
            guess = op_ref[...]
            rest = cross_ref[...] - dot_full(guess, gram_ref[...])
            op_ref[...] = guess + dot3(pieces(rest), pieces(x_ref[...]))
            return carry

        lax.fori_loop(0, 3, again, 0)

    @pl.when(bound_squared > LARGEST_FAST**2)
    def _():
        work[:, :width] = gram_ref[...]
        work[:, width:] = cross_ref[...].T
        eliminate(gram_ref, work, width)
        op_ref[...] = work[:, width:].T

    out = pltpu.make_async_copy(op_ref, op_out, sems.at[0])
    out.start()

    @pl.when(bound_squared > 32.0**2)
    def _():
        seen_ref[...] = dot_full(vectors, op_ref[...], ACROSS)

    residual = seen_ref[...] - values * vectors
    res_ref[...] = residual
    res = pltpu.make_async_copy(res_ref, res_out, sems.at[1])
    res.start()
    sums = jnp.sum(residual * residual, axis=1, keepdims=True)
    sums = jnp.sum(jnp.where(on_diagonal, sums, 0.0), axis=0)
    norm_ref[...] = jnp.sqrt(sums + 1e-06)
    norm = pltpu.make_async_copy(norm_ref, norm_out, sems.at[2])
    norm.start()
    out.wait()
    res.wait()
    norm.wait()


def solve(own, other, gram_own, cross_own, vectors, values, core_of=core_index):
    eigs, width = vectors.shape
    vmem = pl.BlockSpec(memory_space=pltpu.VMEM)
    hbm = pl.BlockSpec(memory_space=pltpu.HBM)
    square = pltpu.VMEM((width, width), jnp.float32)
    return pl.pallas_call(
        functools.partial(solve_kernel, core_of),
        out_shape=(
            jax.ShapeDtypeStruct((width, width), jnp.float32),
            jax.ShapeDtypeStruct((eigs, width), jnp.float32),
            jax.ShapeDtypeStruct((eigs,), jnp.float32),
        ),
        in_specs=[vmem] * 6,
        out_specs=(hbm, hbm, hbm),
        scratch_shapes=[square] * 5
        + [
            pltpu.VMEM((width, 2 * width), jnp.float32),
            pltpu.VMEM((eigs, width), jnp.float32),
            pltpu.VMEM((eigs, width), jnp.float32),
            pltpu.VMEM((eigs,), jnp.float32),
            pltpu.SemaphoreType.DMA((3,)),
        ],
        compiler_params=pltpu.CompilerParams(vmem_limit_bytes=16 * 2**20),
        name="solve",
    )(*map(near, (own, other, gram_own, cross_own, vectors, values)))


def project_kernel(chunk, owner, lines, modes_hbm, snaps_hbm, out, modes_vmem, snaps_vmem, total, mode_sem, snap_sem):
    steps = modes_hbm.shape[0] // chunk

    def copies(step):
        lines = pl.ds(step * chunk, chunk)
        return (
            pltpu.make_async_copy(modes_hbm.at[lines], modes_vmem.at[lines], mode_sem.at[step]),
            pltpu.make_async_copy(snaps_hbm.at[lines], snaps_vmem.at[lines], snap_sem.at[step]),
        )

    for step in range(steps):
        for copy in copies(step):
            copy.start()
    total[...] = jnp.zeros_like(total)

    def add(step, carry):
        for copy in copies(step):
            copy.wait()
        lines = pl.ds(pl.multiple_of(step * chunk, chunk), chunk)
        total[...] += lax.dot_general(
            snaps_vmem[lines, :],
            modes_vmem[lines, :],
            (((0,), (0,)), ((), ())),
            preferred_element_type=jnp.float32,
        )
        return carry

    lax.fori_loop(0, steps, add, 0)
    sums = total[...].T
    for place, block in enumerate(owner):
        out[place] = sums[block * lines : (block + 1) * lines]


def project(modes, snapshots, owner, lines, chunk=2048):
    width, cols = modes.shape[1], snapshots.shape[1]
    steps = modes.shape[0] // chunk
    far = functools.partial(pltpu.with_memory_space_constraint, memory_space=pltpu.HBM)
    return pl.pallas_call(
        functools.partial(project_kernel, chunk, owner, lines),
        out_shape=jax.ShapeDtypeStruct((len(owner), lines, cols), jnp.float32),
        in_specs=[pl.BlockSpec(memory_space=pltpu.HBM)] * 2,
        out_specs=pl.BlockSpec(memory_space=pltpu.VMEM),
        scratch_shapes=[
            pltpu.VMEM(modes.shape, modes.dtype),
            pltpu.VMEM(snapshots.shape, snapshots.dtype),
            pltpu.VMEM((cols, width), jnp.float32),
            pltpu.SemaphoreType.DMA((steps,)),
            pltpu.SemaphoreType.DMA((steps,)),
        ],
        compiler_params=pltpu.CompilerParams(vmem_limit_bytes=40 * 2**20),
        name="project",
    )(far(modes), far(snapshots))


DIMS = "YZzXx"
FIRST = 'ZzXx'
COPIES = 'X'


def plan(rows, times):
    kept = [d for d in DIMS if d in FIRST and d not in COPIES]
    partial = [d for d in DIMS if d not in FIRST]
    places = [dict(zip(DIMS, ((r >> (4 - k)) & 1 for k in range(5)))) for r in range(rows)]

    def packed(place, dims):
        return sum(place[d] << k for k, d in enumerate(reversed(dims)))

    owner = [packed(place, kept) for place in places]
    first, second = {}, {}
    for r, place in enumerate(places):
        first.setdefault(packed(place, partial), []).append(r)
        second.setdefault(packed(place, list(COPIES)), []).append((packed(place, kept + partial), r))
    members = [sorted(first[k], key=lambda r: packed(places[r], 'zxZX')) for k in sorted(first)]
    gathers = [
        [r * times + 2 * low + core for _, r in sorted(second[k]) for low in range(2)]
        for k in sorted(second)
        for core in range(2)
    ]
    return [owner[r] for r in members[0]], members, gathers, 2 ** len(kept), 2 ** len(partial)


def body(snapshots, modes, eig_vectors, eig_values):
    width = modes.shape[1]
    block_cols = snapshots.shape[1]
    rows, times = lax.axis_size("rows"), lax.axis_size("tm")
    owner, members, gathers, owners, parts = plan(rows, times)
    lines = width // owners
    sent = project(modes, snapshots, owner, lines)
    arrived = lax.all_to_all(sent, "rows", 0, 0, tiled=True, axis_index_groups=members)
    own_lines = jnp.sum(arrived, axis=0)
    axes = ("rows", "tm")
    gathered = lax.all_to_all(
        jnp.broadcast_to(own_lines[None], (2 * owners * parts, lines, block_cols)),
        axes,
        0,
        0,
        tiled=True,
        axis_index_groups=gathers,
    )
    if parts > 1:
        gathered = jnp.sum(gathered.reshape(owners, parts, 2, lines, block_cols), axis=1)
    other = lax.ppermute(gathered, axes, [(i, i ^ 1) for i in range(times * rows)])
    shape = (owners, 2, lines, block_cols)
    own, other = gathered.reshape(shape), other.reshape(shape)
    gram_own, cross_own = own_sums(own, width)
    return solve(own, other, gram_own, cross_own, eig_vectors, eig_values)


def solution(mesh):
    return jax.shard_map(
        body,
        mesh=mesh,
        in_specs=(P("rows", "tm"), P("rows", None), P(), P()),
        out_specs=(P(), P(), P()),
        check_vma=False,
    )
```

```python
import functools
import math

import jax
import jax.numpy as jnp
from jax import lax
from jax.experimental import pallas as pl
from jax.experimental.pallas import tpu as pltpu
from jax.sharding import PartitionSpec as P

LARGEST_FAST = 2048.0
RESIDUAL_FLOOR = 150.0
PLAIN = ((1,), (0,))
ACROSS = ((1,), (1,))


def pieces(array):
    high = array.astype(jnp.bfloat16)
    low = (array - high.astype(jnp.float32)).astype(jnp.bfloat16)
    return high, low


def dot3(left, right, contract=PLAIN):
    left_high, left_low = left
    right_high, right_low = right

    def mm(a, b):
        return lax.dot_general(a, b, (contract, ((), ())), preferred_element_type=jnp.float32)

    return mm(left_high, right_high) + (mm(left_high, right_low) + mm(left_low, right_high))


def dot_full(left, right, contract=PLAIN):
    return lax.dot_general(
        left,
        right,
        (contract, ((), ())),
        precision=lax.Precision.HIGHEST,
        preferred_element_type=jnp.float32,
    )


def bound_for(doublings):
    t = RESIDUAL_FLOOR
    for _ in range(doublings + 1):
        t = math.sqrt((t + 1.0) / 2.0)
    return (t + 1.0) / (t - 1.0)


def eliminate(gram_ref, work, width):
    lanes = lax.broadcasted_iota(jnp.int32, (1, 2 * width), 1)
    lines = lax.broadcasted_iota(jnp.int32, (width, 1), 0)

    def step(k, carry):
        row = work[pl.ds(k, 1), :]
        here = (lanes == k).astype(jnp.float32)
        pivot = jnp.sum(row * here, axis=1, keepdims=True)
        row = row / pivot
        column = jnp.sum(work[...] * here, axis=1, keepdims=True)
        on_line = lines == k
        work[...] = jnp.where(on_line, row, work[...] - column * row)
        return carry

    lax.fori_loop(0, width, step, 0)


def core_index():
    return lax.axis_index("tm") & 1


def block_of(ref, half):
    return ref[:, half].reshape(-1, ref.shape[-1])


def half_sums(blocks, drop_last):
    cols = blocks[0].shape[1]
    column = lax.broadcasted_iota(jnp.int32, (1, cols), 1)
    inner = column < cols - 1
    leads = jnp.concatenate(
        [blocks[0], jnp.where(jnp.logical_or(inner, jnp.logical_not(drop_last)), blocks[1], 0.0)],
        axis=1,
    )
    starts = jnp.concatenate([jnp.where(inner, block, 0.0) for block in blocks], axis=1)
    nexts = jnp.concatenate([pltpu.roll(block, cols - 1, 1) for block in blocks], axis=1)
    gram = dot_full(leads, leads, ACROSS)
    cross = dot_full(nexts, starts, ACROSS)
    return gram, cross


def own_kernel(core_of, own_ref, gram_ref, cross_ref):
    blocks = [block_of(own_ref, 0), block_of(own_ref, 1)]
    gram, cross = half_sums(blocks, core_of() == 1)
    gram_ref[...] = gram
    cross_ref[...] = cross


def near(array):
    return pltpu.with_memory_space_constraint(array, pltpu.VMEM)


def own_sums(own, width, core_of=core_index):
    vmem = pl.BlockSpec(memory_space=pltpu.VMEM)
    square = jax.ShapeDtypeStruct((width, width), jnp.float32)
    return pl.pallas_call(
        functools.partial(own_kernel, core_of),
        out_shape=(square, square),
        in_specs=[vmem],
        out_specs=(vmem, vmem),
        compiler_params=pltpu.CompilerParams(vmem_limit_bytes=16 * 2**20),
        cost_estimate=pl.CostEstimate(
            flops=24 * width**3, bytes_accessed=12 * width * width, transcendentals=0
        ),
        name="own_sums",
    )(near(own))


def solve_kernel(core_of, own_ref, other_ref, gram_own_ref, cross_own_ref, vec_ref, val_ref,
                 op_out, res_out, norm_out,
                 gram_ref, cross_ref, r_ref, x_ref, op_ref, work, seen_ref, res_ref, norm_ref, sems):
    width = gram_ref.shape[0]
    core = core_of()
    first = core == 0
    own = [block_of(own_ref, half) for half in range(2)]
    other = [block_of(other_ref, half) for half in range(2)]
    cols = own[0].shape[1]
    scale = 1.0 / (4 * cols - 1)
    eye = (
        lax.broadcasted_iota(jnp.int32, (width, width), 0)
        == lax.broadcasted_iota(jnp.int32, (width, width), 1)
    ).astype(jnp.float32)
    gram_other, cross_other = half_sums(other, first)
    gram = (gram_own_ref[...] + gram_other) * scale + eye
    gram_ref[...] = gram
    gram_pieces = pieces(gram)
    square = dot3(gram_pieces, gram_pieces)

    lane = lax.broadcasted_iota(jnp.int32, (1, cols), 1)
    series = []
    for half in range(2):
        series.append(jnp.where(first, own[half], other[half]))
        series.append(jnp.where(first, other[half], own[half]))
    ends = jnp.zeros_like(series[0])
    begins = jnp.zeros_like(series[0])
    for k in range(3):
        ends = jnp.where(lane == k, pltpu.roll(series[k], k + 1, 1), ends)
        begin = series[k + 1] if k == 0 else pltpu.roll(series[k + 1], k, 1)
        begins = jnp.where(lane == k, begin, begins)
    edges = dot_full(begins, ends, ACROSS)
    cross_ref[...] = (cross_own_ref[...] + cross_other + edges) * scale

    vectors = vec_ref[...]
    eigs = vectors.shape[0]
    on_diagonal = (
        lax.broadcasted_iota(jnp.int32, (eigs, eigs), 0)
        == lax.broadcasted_iota(jnp.int32, (eigs, eigs), 1)
    )
    values = jnp.sum(jnp.where(on_diagonal, val_ref[...][None, :], 0.0), axis=1, keepdims=True)

    top = jnp.max(jnp.sum(jnp.abs(square), axis=0, keepdims=True), axis=1, keepdims=True)
    bound_squared = top[0, 0]
    top = jnp.maximum(jnp.sqrt(top) * 1.001, 1.5)
    doublings = jnp.int32(0)
    for k in range(2, 8):
        doublings += (bound_squared > (bound_for(k) / 1.001) ** 2).astype(jnp.int32)

    @pl.when(bound_squared <= LARGEST_FAST**2)
    def _():
        alpha = 2.0 / (top + 1.0)
        t1 = (top + 1.0) / (top - 1.0)
        t2 = 2.0 * t1 * t1 - 1.0
        i2 = 1.0 / t2
        c = 1.0 + i2
        r2 = c * (eye - (2.0 * alpha) * gram_ref[...] + (alpha * alpha) * square) - i2 * eye
        x2 = (c * alpha) * (2.0 * eye - alpha * gram_ref[...])

        def doubled_x(t, x, rp):
            return (1.0 + 1.0 / t) * (x + dot3(pieces(x), rp))

        def doubled_r(t, rp):
            return (1.0 + 1.0 / t) * dot3(rp, rp) - (1.0 / t) * eye

        t4 = 2.0 * t2 * t2 - 1.0
        rp2 = pieces(r2)
        x_ref[...] = doubled_x(t4, x2, rp2)
        r_ref[...] = doubled_r(t4, rp2)

        def double(_, t):
            t = 2.0 * t * t - 1.0
            rp = pieces(r_ref[...])
            x_ref[...] = doubled_x(t, x_ref[...], rp)
            r_ref[...] = doubled_r(t, rp)
            return t

        t = lax.fori_loop(0, doublings, double, t4)
        t = 2.0 * t * t - 1.0
        x = doubled_x(t, x_ref[...], pieces(r_ref[...]))
        x_ref[...] = x
        xp = pieces(x)

        guess = dot3(pieces(cross_ref[...]), xp)
        seen = dot_full(vectors, guess, ACROSS)
        mixed = dot3(pieces(vectors), xp, ACROSS)
        rest = pieces(cross_ref[...] - dot_full(guess, gram_ref[...]))
        last = 1.0 + 1.0 / (2.0 * t * t - 1.0)
        op_ref[...] = last * (guess + dot3(rest, xp))
        seen_ref[...] = last * (seen + dot3(pieces(mixed), rest, ACROSS))

    @pl.when(jnp.logical_and(bound_squared > 32.0**2, bound_squared <= LARGEST_FAST**2))
    def _():
        def again(_, carry):
            guess = op_ref[...]
            rest = cross_ref[...] - dot_full(guess, gram_ref[...])
            op_ref[...] = guess + dot3(pieces(rest), pieces(x_ref[...]))
            return carry

        lax.fori_loop(0, 3, again, 0)

    @pl.when(bound_squared > LARGEST_FAST**2)
    def _():
        work[:, :width] = gram_ref[...]
        work[:, width:] = cross_ref[...].T
        eliminate(gram_ref, work, width)
        op_ref[...] = work[:, width:].T

    out = pltpu.make_async_copy(op_ref, op_out, sems.at[0])
    out.start()

    @pl.when(bound_squared > 32.0**2)
    def _():
        seen_ref[...] = dot_full(vectors, op_ref[...], ACROSS)

    residual = seen_ref[...] - values * vectors
    res_ref[...] = residual
    res = pltpu.make_async_copy(res_ref, res_out, sems.at[1])
    res.start()
    sums = jnp.sum(residual * residual, axis=1, keepdims=True)
    sums = jnp.sum(jnp.where(on_diagonal, sums, 0.0), axis=0)
    norm_ref[...] = jnp.sqrt(sums + 1e-06)
    norm = pltpu.make_async_copy(norm_ref, norm_out, sems.at[2])
    norm.start()
    out.wait()
    res.wait()
    norm.wait()


def solve(own, other, gram_own, cross_own, vectors, values, core_of=core_index):
    eigs, width = vectors.shape
    vmem = pl.BlockSpec(memory_space=pltpu.VMEM)
    hbm = pl.BlockSpec(memory_space=pltpu.HBM)
    square = pltpu.VMEM((width, width), jnp.float32)
    return pl.pallas_call(
        functools.partial(solve_kernel, core_of),
        out_shape=(
            jax.ShapeDtypeStruct((width, width), jnp.float32),
            jax.ShapeDtypeStruct((eigs, width), jnp.float32),
            jax.ShapeDtypeStruct((eigs,), jnp.float32),
        ),
        in_specs=[vmem] * 6,
        out_specs=(hbm, hbm, hbm),
        scratch_shapes=[square] * 5
        + [
            pltpu.VMEM((width, 2 * width), jnp.float32),
            pltpu.VMEM((eigs, width), jnp.float32),
            pltpu.VMEM((eigs, width), jnp.float32),
            pltpu.VMEM((eigs,), jnp.float32),
            pltpu.SemaphoreType.DMA((3,)),
        ],
        compiler_params=pltpu.CompilerParams(vmem_limit_bytes=16 * 2**20),
        name="solve",
    )(*map(near, (own, other, gram_own, cross_own, vectors, values)))


def project_kernel(chunk, owner, lines, modes_hbm, snaps_hbm, out, modes_vmem, snaps_vmem, total, mode_sem, snap_sem):
    steps = modes_hbm.shape[0] // chunk

    def copies(step):
        lines = pl.ds(step * chunk, chunk)
        return (
            pltpu.make_async_copy(modes_hbm.at[lines], modes_vmem.at[lines], mode_sem.at[step]),
            pltpu.make_async_copy(snaps_hbm.at[lines], snaps_vmem.at[lines], snap_sem.at[step]),
        )

    for step in range(steps):
        for copy in copies(step):
            copy.start()
    total[...] = jnp.zeros_like(total)

    def add(step, carry):
        for copy in copies(step):
            copy.wait()
        lines = pl.ds(pl.multiple_of(step * chunk, chunk), chunk)
        total[...] += lax.dot_general(
            snaps_vmem[lines, :],
            modes_vmem[lines, :],
            (((0,), (0,)), ((), ())),
            preferred_element_type=jnp.float32,
        )
        return carry

    lax.fori_loop(0, steps, add, 0)
    sums = total[...].T
    for place, block in enumerate(owner):
        out[place] = sums[block * lines : (block + 1) * lines]


def project(modes, snapshots, owner, lines, chunk=2048):
    width, cols = modes.shape[1], snapshots.shape[1]
    steps = modes.shape[0] // chunk
    far = functools.partial(pltpu.with_memory_space_constraint, memory_space=pltpu.HBM)
    return pl.pallas_call(
        functools.partial(project_kernel, chunk, owner, lines),
        out_shape=jax.ShapeDtypeStruct((len(owner), lines, cols), jnp.float32),
        in_specs=[pl.BlockSpec(memory_space=pltpu.HBM)] * 2,
        out_specs=pl.BlockSpec(memory_space=pltpu.VMEM),
        scratch_shapes=[
            pltpu.VMEM(modes.shape, modes.dtype),
            pltpu.VMEM(snapshots.shape, snapshots.dtype),
            pltpu.VMEM((cols, width), jnp.float32),
            pltpu.SemaphoreType.DMA((steps,)),
            pltpu.SemaphoreType.DMA((steps,)),
        ],
        compiler_params=pltpu.CompilerParams(vmem_limit_bytes=40 * 2**20),
        name="project",
    )(far(modes), far(snapshots))


DIMS = "YZzXx"
FIRST = 'ZzXx'
COPIES = 'X'


def plan(rows, times):
    kept = [d for d in DIMS if d in FIRST and d not in COPIES]
    partial = [d for d in DIMS if d not in FIRST]
    places = [dict(zip(DIMS, ((r >> (4 - k)) & 1 for k in range(5)))) for r in range(rows)]

    def packed(place, dims):
        return sum(place[d] << k for k, d in enumerate(reversed(dims)))

    owner = [packed(place, kept) for place in places]
    first, second = {}, {}
    for r, place in enumerate(places):
        first.setdefault(packed(place, partial), []).append(r)
        second.setdefault(packed(place, list(COPIES)), []).append((packed(place, kept + partial), r))
    members = [sorted(first[k], key=lambda r: packed(places[r], 'zxZX')) for k in sorted(first)]
    gathers = [
        [r * times + 2 * low + core for _, r in sorted(second[k]) for low in range(2)]
        for k in sorted(second)
        for core in range(2)
    ]
    return [owner[r] for r in members[0]], members, gathers, 2 ** len(kept), 2 ** len(partial)


def body(snapshots, modes, eig_vectors, eig_values):
    width = modes.shape[1]
    block_cols = snapshots.shape[1]
    rows, times = lax.axis_size("rows"), lax.axis_size("tm")
    owner, members, gathers, owners, parts = plan(rows, times)
    lines = width // owners
    sent = project(modes, snapshots, owner, lines)
    arrived = lax.all_to_all(sent, "rows", 0, 0, tiled=True, axis_index_groups=members)
    own_lines = jnp.sum(arrived, axis=0)
    axes = ("rows", "tm")
    gathered = lax.all_to_all(
        jnp.broadcast_to(own_lines[None], (2 * owners * parts, lines, block_cols)),
        axes,
        0,
        0,
        tiled=True,
        axis_index_groups=gathers,
    )
    if parts > 1:
        gathered = jnp.sum(gathered.reshape(owners, parts, 2, lines, block_cols), axis=1)
    other = lax.ppermute(gathered, axes, [(i, i ^ 1) for i in range(times * rows)])
    shape = (owners, 2, lines, block_cols)
    own, other = gathered.reshape(shape), other.reshape(shape)
    gram_own, cross_own = own_sums(own, width)
    return solve(own, other, gram_own, cross_own, eig_vectors, eig_values)


def solution(mesh):
    return jax.shard_map(
        body,
        mesh=mesh,
        in_specs=(P("rows", "tm"), P("rows", None), P(), P()),
        out_specs=(P(), P(), P()),
        check_vma=False,
    )
```
